256 devices in a mesh: grp: 4 (over y), dev: 64 (over z, x, core).
Axes of the slice: x: 4, y: 4, z: 8, core: 2. Of those that a mesh axis runs over, the one named last changes fastest.
Arguments:
- nz_user: int32 [32768, 128], P(('grp', 'dev')), may hold values from 0 to 65535
- nz_sub: int32 [32768, 128], P(('grp', 'dev')), may hold values from 0 to 16383
- nz_value: float32 [32768, 128], P(('grp', 'dev')), may hold values from -1 to 1
- tile_word: int32 [32768], P(('grp', 'dev')), may hold values from 0 to 16383, as said below
- word_owner: int32 [16384], replicated, may hold values from 0 to 16383, as said below
- user_factor: bfloat16 [64, 65536], P(None, 'dev'), may hold values from -6 to 6
- sub_factor: bfloat16 [64, 16384], P(None, 'dev'), may hold values from -6 to 6
Outputs:
- word_rows: float32 [64, 16384], P(None, ('grp', 'dev'))
The draws below stay inside these ranges and needn't reach their ends.
Inputs may be any that keep to these rules, and one draw needn't show every extreme that they name: A permutation of the word indices: word w is summed into column word_owner[w] of word_rows. `tile_word`: tile i lies on device i // 128 (grp+dev order). On every device at most 2 tiles belong to words whose output column lies on any one other device, and on every device that bound is reached for some other device.
All inputs are finite; a program needn't handle non-finite values.
Results may differ from the reference program's by a relative error of at most 0.0003.
Values may be sent and summed in bfloat16 or wider, within the bound.
No kernel may reach another device: no remote copies, remote signals or barrier semaphores. Data moves between devices by JAX's collectives and lax.ppermute only.
A program may use at most 64 MiB of HBM per device.

```python
import math
import jax
import jax.numpy as jnp
import numpy as np
from jax import lax

RANK = 64
NZ = 128
CAP = 2
TILES_DEV = 128
WORDS_DEV = 64
TILES = 32768
USERS = 65536
SUBS = 16384
WORDS = 16384


def layout(key):
    devices_all = TILES // TILES_DEV
    owner_key = jax.random.fold_in(key, 11)
    word_owner = jax.random.permutation(owner_key, WORDS).astype(jnp.int32)
    word_of_row = jnp.zeros((WORDS,), jnp.int32).at[word_owner].set(jnp.arange(WORDS, dtype=jnp.int32))
    heavy_count = min(4, WORDS_DEV)
    heavy_key = jax.random.fold_in(key, 17)

    def heavy_rows(device_index):
        return jax.random.permutation(jax.random.fold_in(heavy_key, device_index), WORDS_DEV)[:heavy_count].astype(jnp.int32)
    heavy_table = jax.vmap(heavy_rows)(jnp.arange(devices_all, dtype=jnp.int32))

    def one_device(device_index):
        device_key = jax.random.fold_in(jax.random.fold_in(key, 23), device_index)
        key_list = jax.random.split(device_key, 6)
        hot_device = (device_index + 1 + jax.random.randint(key_list[0], (), 0, devices_all - 1)) % devices_all
        pair_ids = jnp.arange(devices_all * CAP, dtype=jnp.int32)
        pair_target = pair_ids // CAP
        order_key = jax.random.permutation(key_list[1], devices_all * CAP).astype(jnp.int32)
        order_key = jnp.where(pair_target == hot_device, -1 - pair_ids % CAP, order_key)
        pair_order = pair_target[jnp.argsort(order_key, stable=True)]
        remote_count = jnp.minimum(jax.random.randint(key_list[2], (), 3 * TILES_DEV // 16, 3 * TILES_DEV // 8 + 1), devices_all * CAP)
        slot_ids = jnp.arange(TILES_DEV, dtype=jnp.int32)
        padded_order = pair_order[jnp.minimum(slot_ids, devices_all * CAP - 1)]
        destination = jnp.where(slot_ids < remote_count, padded_order, device_index).astype(jnp.int32)
        heavy_pick = jax.random.randint(key_list[3], (TILES_DEV,), 0, heavy_count)
        light_pick = jax.random.randint(key_list[4], (TILES_DEV,), 0, WORDS_DEV)
        offset = jnp.where(destination == device_index, light_pick, heavy_table[destination, heavy_pick]).astype(jnp.int32)
        words = word_of_row[destination * WORDS_DEV + offset]
        shuffle = jax.random.permutation(key_list[5], TILES_DEV)
        return words[shuffle].astype(jnp.int32)
    tile_word = jax.vmap(one_device)(jnp.arange(devices_all, dtype=jnp.int32)).reshape(TILES)
    return (word_owner, tile_word)


def draw_word_owner(key, part):
    return layout(key)[0]


def draw_tile_word(key, part):
    return layout(key)[1]


def draw_nz_value(key, part):
    key_list = jax.random.split(jax.random.fold_in(key, 37), 3)
    live_count = jax.random.randint(key_list[0], (TILES, 1), NZ // 4, NZ + 1)
    filled = (jnp.arange(NZ)[None, :] < live_count).astype(jnp.float32)
    raw_values = 0.125 * jax.random.normal(key_list[2], (TILES, NZ))
    return (jnp.clip(raw_values, -1.0, 1.0) * filled).astype(jnp.float32)


def place_ends(result, key, least, high):
    place = [jax.random.randint(jax.random.fold_in(key, axis), (), 0, length) for axis, length in enumerate(result.shape)]
    longest = result.shape.index(max(result.shape))
    next_to = place[:longest] + [(place[longest] + 1) % result.shape[longest]] + place[longest + 1:]
    return result.at[tuple(place)].set(least).at[tuple(next_to)].set(high)


def levels(rng, dims, cuts, least, largest):
    def one(dim, blocks):
        draws = jax.random.uniform(jax.random.fold_in(jax.random.fold_in(rng, 6), dim), (blocks,), jnp.float32, least / len(cuts), largest / len(cuts))
        return jnp.repeat(jnp.exp(draws), dims[dim] // blocks).reshape((-1,) + (1,) * (len(dims) - dim - 1))

    factor_of = one(*cuts[0])
    for cut in cuts[1:]:
        factor_of = factor_of * one(*cut)
    return factor_of


def rank_bounds(amount, slope):
    portions = [(1 << 20) // math.isqrt(standing ** slope) + 1 for standing in range(1, amount + 1)]
    deviation = 1 + sum(portions) // (1 << 30)
    return np.cumsum(np.array([max(1, weight // deviation) for weight in portions]))


def skewed_ids(key, dims, number_of, lean):
    listing = rank_bounds(number_of, lean)
    lot = jax.random.randint(jax.random.fold_in(key, 1), dims, 0, int(listing[number_of - 1]))
    rank = jnp.searchsorted(jnp.asarray(listing, jnp.int32), lot, side="right")
    return jax.random.permutation(jax.random.fold_in(key, 2), number_of)[rank].astype(jnp.int32)


def bell_draw(own_key, shape, deviation, limit, cuts=(), held_as=jnp.bfloat16):
    entries = deviation * jax.random.normal(own_key, shape, jnp.float32)
    if cuts:
        entries = entries * levels(own_key, shape, cuts, -0.22, 0.18)
    return jnp.clip(entries, -limit, limit).astype(held_as)


def setup_inputs(seed: int = 0) -> dict:
    seeds = jax.random.split(jax.random.key(seed), 8)
    return {
        "nz_user": place_ends(jax.random.randint(seeds[0], (TILES, NZ), 0, USERS), jax.random.fold_in(seeds[0], 1), 0, USERS - 1).astype(jnp.int32),
        "nz_sub": place_ends(skewed_ids(seeds[1], (TILES, NZ), SUBS, 2), jax.random.fold_in(seeds[1], 3), 0, SUBS - 1).astype(jnp.int32),
        "nz_value": draw_nz_value(jax.random.fold_in(seeds[7], 71), 0),
        "tile_word": draw_tile_word(jax.random.fold_in(seeds[7], 71), 0),
        "word_owner": draw_word_owner(jax.random.fold_in(seeds[7], 71), 0),
        "user_factor": bell_draw(seeds[5], (RANK, USERS), 1.0, 6.0, ((1, 64),)),
        "sub_factor": bell_draw(seeds[6], (RANK, SUBS), 1.0, 6.0, ((1, 64),)),
    }


def reference(nz_user, nz_sub, nz_value, tile_word, word_owner, user_factor, sub_factor):
    tile_total, tile_width = nz_user.shape
    block_tiles = min(tile_total, 256)
    block_count = tile_total // block_tiles

    def one_block(block_args):
        users_block, subs_block, vals_block = block_args
        user_cols = jnp.take(user_factor, users_block, axis=1).astype(jnp.float32)
        sub_cols = jnp.take(sub_factor, subs_block, axis=1).astype(jnp.float32)
        return jnp.sum(user_cols * sub_cols * vals_block[None], axis=2)

    block_sums = lax.map(one_block, (nz_user.reshape(block_count, block_tiles, tile_width),
                                     nz_sub.reshape(block_count, block_tiles, tile_width),
                                     nz_value.reshape(block_count, block_tiles, tile_width)))
    partial_value = jnp.transpose(block_sums, (1, 0, 2)).reshape(block_sums.shape[1], tile_total)
    out_rows = jnp.take(word_owner, tile_word)
    return jnp.zeros((partial_value.shape[0], WORDS), jnp.float32).at[:, out_rows].add(partial_value)
```

```python
import functools

import jax
import jax.numpy as jnp
from jax import lax
from jax.experimental import pallas as pl
from jax.experimental.pallas import tpu as pltpu
from jax.sharding import PartitionSpec as P

CAP = 2


def cut_along(value, dim, peers):
    shape = value.shape
    pieces = value.reshape(*shape[:dim], peers, shape[dim] // peers, *shape[dim + 1 :])
    return jnp.moveaxis(pieces, dim, 0)


def joined_along(pieces, dim):
    pieces = jnp.moveaxis(pieces, 0, dim)
    shape = pieces.shape
    return pieces.reshape(*shape[:dim], shape[dim] * shape[dim + 1], *shape[dim + 2 :])


def exchange_both(value, axis, axes, splits, concats):
    sizes = [lax.axis_size(a) for a in axes]
    pieces = cut_along(value, splits[0], sizes[0])
    pieces = jnp.moveaxis(cut_along(pieces, splits[1] + 1, sizes[1]), 0, 1)
    inside = pieces.shape[2:]
    pieces = pieces.reshape(-1, *inside)
    pieces = lax.all_to_all(pieces, axis, split_axis=0, concat_axis=0, tiled=True)
    pieces = joined_along(pieces.reshape(*sizes, *inside), concats[0] + 1)
    return joined_along(pieces, concats[1])


NT = 8
CH = NT * 128
BLOCK = 640


def merged(rows):
    sublane = lax.broadcasted_iota(jnp.int32, (8, 128), 0)
    out = jnp.broadcast_to(rows[0], (8, 128))
    for k in range(1, 8):
        out = jnp.where(sublane == k, jnp.broadcast_to(rows[k], (8, 128)), out)
    return out


def tile_kernel(devs, tiles, idx_hbm, w0_ref, w1_ref, tab_hbm, out_ref, utab, stab, stage, bufa, bufb, sem, isem):
    f32 = jnp.float32
    bufs = (bufa, bufb)
    steps = tiles // (2 * NT)

    def icopy(c, b):
        return pltpu.make_async_copy(idx_hbm.at[pl.ds(c * 2 * CH, 2 * CH)], bufs[b], isem.at[b])

    icopy(0, 0).start()
    icopy(1, 1).start()

    def tcopy(d):
        rows = pl.ds(pl.multiple_of(d * BLOCK, 128), BLOCK)
        return pltpu.make_async_copy(tab_hbm.at[rows, :], stage.at[rows, :], sem.at[d])

    for d in range(devs):
        tcopy(d).start()
    low = lax.broadcasted_iota(jnp.int32, (128, 128), 1) < 64

    def conv(d, carry):
        tcopy(d).wait()
        base = pl.multiple_of(d * BLOCK, 128)
        utab[pl.ds(pl.multiple_of(d * 512, 512), 512), :] = stage[pl.ds(base, 512), :].astype(f32)
        x = stage[pl.ds(base + 512, 128), :].astype(f32)
        r = pltpu.roll(x, 64, 1)
        stab[pl.ds(pl.multiple_of(d * 256, 256), 128), :] = jnp.where(low, x, r)
        stab[pl.ds(pl.multiple_of(d * 256 + 128, 128), 128), :] = jnp.where(low, r, x)
        return carry

    lax.fori_loop(0, devs, conv, 0)

    def tile(buf, j, t):
        w0 = w0_ref[pl.ds(t, 1), :]
        w1 = w1_ref[pl.ds(t, 1), :]
        w = jnp.concatenate([jnp.broadcast_to(w0, (64, 128)), jnp.broadcast_to(w1, (64, 128))], 0).T
        acc = jnp.zeros((8, 128), f32)
        for g in range(16):
            first = j * 128 + g * 8
            ur = merged([utab[pl.ds(buf[first + k], 1), :] for k in range(8)])
            sr = merged([stab[pl.ds(buf[CH + first + k], 1), :] for k in range(8)])
            acc = acc + ur * sr * w[g * 8 : (g + 1) * 8, :]
        out_ref[pl.ds(t, 1), :] = jnp.sum(acc, axis=0, keepdims=True)

    def body(i, carry):
        for b in range(2):
            c = i * 2 + b
            icopy(c, b).wait()
            for j in range(NT):
                tile(bufs[b], j, c * NT + j)

            @pl.when(i < steps - 1)
            def _():
                icopy(c + 2, b).start()

        return carry

    lax.fori_loop(0, steps, body, 0)


def tile_sums(table, nz_user, nz_sub, nz_value):
    tiles, width = nz_user.shape
    devs = lax.axis_size("dev")
    user_row = (nz_user >> 10) * 512 + (nz_user & 511)
    high = ((nz_user >> 9) & 1) == 1
    w1 = jnp.where(high, nz_value, 0.0)
    w0 = jnp.where(high, 0.0, nz_value)
    idx = jnp.concatenate([user_row.reshape(-1, 1, CH), nz_sub.reshape(-1, 1, CH)], axis=1).reshape(-1)
    out = pl.pallas_call(
        functools.partial(tile_kernel, devs, tiles),
        out_shape=jax.ShapeDtypeStruct((tiles, 128), jnp.float32),
        in_specs=[
            pl.BlockSpec(memory_space=pltpu.HBM),
            pl.BlockSpec(memory_space=pltpu.VMEM),
            pl.BlockSpec(memory_space=pltpu.VMEM),
            pl.BlockSpec(memory_space=pltpu.HBM),
        ],
        out_specs=pl.BlockSpec(memory_space=pltpu.VMEM),
        scratch_shapes=[
            pltpu.VMEM((devs * 512, 128), jnp.float32),
            pltpu.VMEM((devs * 256, 128), jnp.float32),
            pltpu.VMEM((devs * BLOCK, 128), jnp.bfloat16),
            pltpu.SMEM((2 * CH,), jnp.int32),
            pltpu.SMEM((2 * CH,), jnp.int32),
            pltpu.SemaphoreType.DMA((devs,)),
            pltpu.SemaphoreType.DMA((2,)),
        ],
        compiler_params=pltpu.CompilerParams(vmem_limit_bytes=44 * 2**20),
        name="tile_sums",
    )(idx, w0, w1, table)
    return out[:, :64] + out[:, 64:]


def packed(factor):
    rows = jnp.transpose(factor)
    half = rows.shape[0] // 2
    return jnp.concatenate([rows[:half], rows[half:]], axis=1)


def shards(nz_user, nz_sub, nz_value, tile_word, word_owner, user_factor, sub_factor):
    mine = jnp.concatenate([packed(user_factor), packed(sub_factor)], axis=0)
    table = lax.all_gather(mine, "dev", axis=0, tiled=True)
    tile_rows = tile_sums(table, nz_user, nz_sub, nz_value)
    tile_count, rank_width = tile_rows.shape
    grp_size = lax.axis_size("grp")
    dev_size = lax.axis_size("dev")
    devices_all = grp_size * dev_size
    words_total = word_owner.shape[0]
    words_local = words_total // devices_all
    out_rows = jnp.take(word_owner, tile_word)
    self_index = lax.axis_index("grp") * dev_size + lax.axis_index("dev")
    owner_dev = out_rows // words_local
    local_row = out_rows - owner_dev * words_local
    owned = owner_dev == self_index
    columns = jnp.arange(words_local, dtype=jnp.int32)
    own_table = (owned[:, None] & (local_row[:, None] == columns[None, :])).astype(jnp.float32)
    own_part = jnp.einsum("tr,tk->rk", tile_rows, own_table, precision=lax.Precision.HIGHEST)
    peer_ids = jnp.arange(devices_all, dtype=jnp.int32)
    outgoing = (jnp.logical_not(owned)[:, None] & (owner_dev[:, None] == peer_ids[None, :])).astype(
        jnp.float32
    )
    tile_ids = jnp.arange(tile_count, dtype=jnp.int32)
    earlier_table = (tile_ids[:, None] > tile_ids[None, :]).astype(jnp.float32)
    earlier = jnp.dot(
        earlier_table, outgoing, precision=lax.Precision.HIGHEST, preferred_element_type=jnp.float32
    )
    position = jnp.sum(earlier * outgoing, axis=1).astype(jnp.int32)
    send_slot = jnp.where(owned, devices_all * CAP, owner_dev * CAP + position)
    slot_ids = jnp.arange(devices_all * CAP, dtype=jnp.int32)
    slot_table = (send_slot[:, None] == slot_ids[None, :]).astype(jnp.float32)
    send_rows = jnp.einsum("ts,tr->sr", slot_table, tile_rows, precision=lax.Precision.HIGHEST)
    filled = jnp.sum(slot_table, axis=0)
    send_ids = (
        jnp.dot(
            local_row.astype(jnp.float32),
            slot_table,
            precision=lax.Precision.HIGHEST,
            preferred_element_type=jnp.float32,
        )
        + filled
        - 1.0
    )
    send_rows = send_rows.reshape(grp_size, dev_size, CAP * rank_width)
    send_ids = send_ids.reshape(grp_size, dev_size, CAP)
    got_rows, got_ids = (
        exchange_both(send_rows, ("dev", "grp"), ("dev", "grp"), (1, 0), (1, 0)),
        exchange_both(send_ids, ("dev", "grp"), ("dev", "grp"), (1, 0), (1, 0)),
    )
    got_rows = got_rows.reshape(devices_all * CAP, rank_width)
    got_ids = got_ids.reshape(devices_all * CAP).astype(jnp.int32)
    got_table = (got_ids[:, None] == columns[None, :]).astype(jnp.float32)
    far_part = jnp.einsum("sr,sk->rk", got_rows, got_table, precision=lax.Precision.HIGHEST)
    return own_part + far_part


def solution(mesh):
    return jax.shard_map(
        shards,
        mesh=mesh,
        in_specs=(
            P(("grp", "dev"), None),
            P(("grp", "dev"), None),
            P(("grp", "dev"), None),
            P(("grp", "dev")),
            P(),
            P(None, "dev"),
            P(None, "dev"),
        ),
        out_specs=P(None, ("grp", "dev")),
        check_vma=False,
    )
```

```python
import functools

import jax
import jax.numpy as jnp
from jax import lax
from jax.experimental import pallas as pl
from jax.experimental.pallas import tpu as pltpu
from jax.sharding import PartitionSpec as P

CAP = 2


def cut_along(value, dim, peers):
    shape = value.shape
    pieces = value.reshape(*shape[:dim], peers, shape[dim] // peers, *shape[dim + 1 :])
    return jnp.moveaxis(pieces, dim, 0)


def joined_along(pieces, dim):
    pieces = jnp.moveaxis(pieces, 0, dim)
    shape = pieces.shape
    return pieces.reshape(*shape[:dim], shape[dim] * shape[dim + 1], *shape[dim + 2 :])


def exchange_both(value, axis, axes, splits, concats):
    sizes = [lax.axis_size(a) for a in axes]
    pieces = cut_along(value, splits[0], sizes[0])
    pieces = jnp.moveaxis(cut_along(pieces, splits[1] + 1, sizes[1]), 0, 1)
    inside = pieces.shape[2:]
    pieces = pieces.reshape(-1, *inside)
    pieces = lax.all_to_all(pieces, axis, split_axis=0, concat_axis=0, tiled=True)
    pieces = joined_along(pieces.reshape(*sizes, *inside), concats[0] + 1)
    return joined_along(pieces, concats[1])


NT = 8
CH = NT * 128
SHARD_U = 256
SHARD_S = 64
SHARD = SHARD_U + SHARD_S


def merged(rows):
    sublane = lax.broadcasted_iota(jnp.int32, (8, 128), 0)
    out = jnp.broadcast_to(rows[0], (8, 128))
    for k in range(1, 8):
        out = jnp.where(sublane == k, jnp.broadcast_to(rows[k], (8, 128)), out)
    return out


def tile_kernel(counts, tiles, idx_hbm, w0_ref, w1_ref, *refs):
    f32 = jnp.float32
    pieces, (out_ref, utab, stab, bufa, bufb, isem) = refs[: len(counts)], refs[len(counts) :]
    bufs = (bufa, bufb)
    steps = tiles // (2 * NT)

    def icopy(c, b):
        return pltpu.make_async_copy(idx_hbm.at[pl.ds(c * 2 * CH, 2 * CH)], bufs[b], isem.at[b])

    icopy(0, 0).start()
    icopy(1, 1).start()
    low = lax.broadcasted_iota(jnp.int32, (SHARD_S, 128), 1) < 64
    first_slot = 0
    for piece, count in zip(pieces, counts):

        def conv(i, carry, piece=piece, first_slot=first_slot):
            src = pl.multiple_of(i * SHARD, SHARD_S)
            slot = first_slot + i
            urow = pl.multiple_of(slot * SHARD_U, SHARD_U)
            srow = pl.multiple_of(slot * 2 * SHARD_S, 2 * SHARD_S)
            utab[pl.ds(urow, SHARD_U), :] = piece[pl.ds(src, SHARD_U), :].astype(f32)
            x = piece[pl.ds(src + SHARD_U, SHARD_S), :].astype(f32)
            r = pltpu.roll(x, 64, 1)
            stab[pl.ds(srow, SHARD_S), :] = jnp.where(low, x, r)
            stab[pl.ds(srow + SHARD_S, SHARD_S), :] = jnp.where(low, r, x)
            return carry

        lax.fori_loop(0, count, conv, 0)
        first_slot += count

    def tile(buf, j, t):
        w0 = w0_ref[pl.ds(t, 1), :]
        w1 = w1_ref[pl.ds(t, 1), :]
        w = jnp.concatenate([jnp.broadcast_to(w0, (64, 128)), jnp.broadcast_to(w1, (64, 128))], 0).T
        acc = jnp.zeros((8, 128), f32)
        for g in range(16):
            first = j * 128 + g * 8
            ur = merged([utab[pl.ds(buf[first + k], 1), :] for k in range(8)])
            sr = merged([stab[pl.ds(buf[CH + first + k], 1), :] for k in range(8)])
            acc = acc + ur * sr * w[g * 8 : (g + 1) * 8, :]
        out_ref[pl.ds(t, 1), :] = jnp.sum(acc, axis=0, keepdims=True)

    def body(i, carry):
        for b in range(2):
            c = i * 2 + b
            icopy(c, b).wait()
            for j in range(NT):
                tile(bufs[b], j, c * NT + j)

            @pl.when(i < steps - 1)
            def _():
                icopy(c + 2, b).start()

        return carry

    lax.fori_loop(0, steps, body, 0)


def slot_of(dev, color):
    me = lax.axis_index("dev")
    dz = ((dev >> 3) - (me >> 3)) & 7
    dx = ((dev >> 1) - (me >> 1)) & 3
    other = (dev ^ me) & 1
    return (color * 2 + other) * 32 + jnp.where(color == 1, dx * 8 + dz, dz * 4 + dx)


def tile_sums(pieces, nz_user, nz_sub, nz_value):
    tiles, width = nz_user.shape
    counts = tuple(p.shape[0] // SHARD for p in pieces)
    slots = sum(counts)
    user_row = slot_of(nz_user >> 10, (nz_user >> 8) & 1) * SHARD_U + (nz_user & 255)
    sub_row = (slot_of(nz_sub >> 8, (nz_sub >> 6) & 1) * 2 + ((nz_sub >> 7) & 1)) * SHARD_S + (nz_sub & 63)
    high = ((nz_user >> 9) & 1) == 1
    w1 = jnp.where(high, nz_value, 0.0)
    w0 = jnp.where(high, 0.0, nz_value)
    idx = jnp.concatenate([user_row.reshape(-1, 1, CH), sub_row.reshape(-1, 1, CH)], axis=1).reshape(-1)
    vmem = pl.BlockSpec(memory_space=pltpu.VMEM)
    out = pl.pallas_call(
        functools.partial(tile_kernel, counts, tiles),
        out_shape=jax.ShapeDtypeStruct((tiles, 128), jnp.float32),
        in_specs=[pl.BlockSpec(memory_space=pltpu.HBM), vmem, vmem] + [vmem] * len(pieces),
        out_specs=vmem,
        scratch_shapes=[
            pltpu.VMEM((slots * SHARD_U, 128), jnp.float32),
            pltpu.VMEM((slots * 2 * SHARD_S, 128), jnp.float32),
            pltpu.SMEM((2 * CH,), jnp.int32),
            pltpu.SMEM((2 * CH,), jnp.int32),
            pltpu.SemaphoreType.DMA((2,)),
        ],
        compiler_params=pltpu.CompilerParams(vmem_limit_bytes=44 * 2**20),
        name="tile_sums",
    )(idx, w0, w1, *pieces)
    return out[:, :64] + out[:, 64:]


def sent(value, dz, dx, dc=0):
    devs = lax.axis_size("dev")
    pairs = [(d, ((d // 8 + dz) % 8) * 8 + ((d % 8 // 2 + dx) % 4) * 2 + ((d % 2) ^ dc)) for d in range(devs)]
    return lax.ppermute(value, "dev", pairs)


def along_z(block):
    half = block.shape[0] // 2
    up, down = [], []
    p = m = block
    for _ in range(3):
        p, m = sent(p, 1, 0), sent(m, -1, 0)
        up.append(p)
        down.append(m)
    return [block] + down + [sent(p[:half], 1, 0), sent(m[half:], -1, 0)] + up[::-1]


def gathered(mine_a, mine_b):
    block_a = jnp.concatenate([mine_a, sent(mine_a, 0, -1), sent(mine_a, 0, 2), sent(mine_a, 0, 1)], axis=0)
    pieces_a = along_z(block_a)
    block_b = jnp.concatenate(along_z(mine_b), axis=0)
    half = block_b.shape[0] // 2
    p, m = sent(block_b, 0, 1), sent(block_b, 0, -1)
    pieces_b = [block_b, m, sent(p[:half], 0, 1), sent(m[half:], 0, -1), p]
    other_a = [sent(v, 0, 0, 1) for v in pieces_a]
    other_b = [sent(v, 0, 0, 1) for v in pieces_b]
    return pieces_a + other_a + pieces_b + other_b


def packed(factor):
    rows = jnp.transpose(factor)
    half = rows.shape[0] // 2
    return jnp.concatenate([rows[:half], rows[half:]], axis=1)


def shards(nz_user, nz_sub, nz_value, tile_word, word_owner, user_factor, sub_factor):
    users, subs = packed(user_factor), packed(sub_factor)
    mine_a = jnp.concatenate([users[:SHARD_U], subs[:SHARD_S]], axis=0)
    mine_b = jnp.concatenate([users[SHARD_U:], subs[SHARD_S:]], axis=0)
    tile_rows = tile_sums(gathered(mine_a, mine_b), nz_user, nz_sub, nz_value)
    tile_count, rank_width = tile_rows.shape
    grp_size = lax.axis_size("grp")
    dev_size = lax.axis_size("dev")
    devices_all = grp_size * dev_size
    words_total = word_owner.shape[0]
    words_local = words_total // devices_all
    out_rows = jnp.take(word_owner, tile_word)
    self_index = lax.axis_index("grp") * dev_size + lax.axis_index("dev")
    owner_dev = out_rows // words_local
    local_row = out_rows - owner_dev * words_local
    owned = owner_dev == self_index
    columns = jnp.arange(words_local, dtype=jnp.int32)
    own_table = (owned[:, None] & (local_row[:, None] == columns[None, :])).astype(jnp.float32)
    own_part = jnp.einsum("tr,tk->rk", tile_rows, own_table, precision=lax.Precision.HIGHEST)
    peer_ids = jnp.arange(devices_all, dtype=jnp.int32)
    outgoing = (jnp.logical_not(owned)[:, None] & (owner_dev[:, None] == peer_ids[None, :])).astype(
        jnp.float32
    )
    tile_ids = jnp.arange(tile_count, dtype=jnp.int32)
    earlier_table = (tile_ids[:, None] > tile_ids[None, :]).astype(jnp.float32)
    earlier = jnp.dot(
        earlier_table, outgoing, precision=lax.Precision.HIGHEST, preferred_element_type=jnp.float32
    )
    position = jnp.sum(earlier * outgoing, axis=1).astype(jnp.int32)
    send_slot = jnp.where(owned, devices_all * CAP, owner_dev * CAP + position)
    slot_ids = jnp.arange(devices_all * CAP, dtype=jnp.int32)
    slot_table = (send_slot[:, None] == slot_ids[None, :]).astype(jnp.float32)
    with_ids = jnp.concatenate(
        [tile_rows, (local_row + 1).astype(jnp.float32)[:, None], jnp.zeros((tile_count, 127 - rank_width), jnp.float32)],
        axis=1,
    )
    send = jnp.einsum("ts,tr->sr", slot_table, with_ids, precision=lax.Precision.HIGHEST)
    send = send.reshape(grp_size, dev_size, CAP * 128)
    got = exchange_both(send, ("dev", "grp"), ("dev", "grp"), (1, 0), (1, 0))
    got = got.reshape(devices_all * CAP, 128)
    got_rows = got[:, :rank_width]
    got_ids = got[:, rank_width].astype(jnp.int32) - 1
    got_table = (got_ids[:, None] == columns[None, :]).astype(jnp.float32)
    far_part = jnp.einsum("sr,sk->rk", got_rows, got_table, precision=lax.Precision.HIGHEST)
    return own_part + far_part


def solution(mesh):
    return jax.shard_map(
        shards,
        mesh=mesh,
        in_specs=(
            P(("grp", "dev"), None),
            P(("grp", "dev"), None),
            P(("grp", "dev"), None),
            P(("grp", "dev")),
            P(),
            P(None, "dev"),
            P(None, "dev"),
        ),
        out_specs=P(None, ("grp", "dev")),
        check_vma=False,
    )
```

```python
import functools

import jax
import jax.numpy as jnp
from jax import lax
from jax.experimental import pallas as pl
from jax.experimental.pallas import tpu as pltpu
from jax.sharding import PartitionSpec as P

CAP = 2


def cut_along(value, dim, peers):
    shape = value.shape
    pieces = value.reshape(*shape[:dim], peers, shape[dim] // peers, *shape[dim + 1 :])
    return jnp.moveaxis(pieces, dim, 0)


def joined_along(pieces, dim):
    pieces = jnp.moveaxis(pieces, 0, dim)
    shape = pieces.shape
    return pieces.reshape(*shape[:dim], shape[dim] * shape[dim + 1], *shape[dim + 2 :])


def exchange_both(value, axis, axes, splits, concats):
    sizes = [lax.axis_size(a) for a in axes]
    pieces = cut_along(value, splits[0], sizes[0])
    pieces = jnp.moveaxis(cut_along(pieces, splits[1] + 1, sizes[1]), 0, 1)
    inside = pieces.shape[2:]
    pieces = pieces.reshape(-1, *inside)
    pieces = lax.all_to_all(pieces, axis, split_axis=0, concat_axis=0, tiled=True)
    pieces = joined_along(pieces.reshape(*sizes, *inside), concats[0] + 1)
    return joined_along(pieces, concats[1])


NT = 8
CH = NT * 128
SHARD_U = 256
SHARD_S = 64
SHARD = SHARD_U + SHARD_S


def merged(rows):
    sublane = lax.broadcasted_iota(jnp.int32, (8, 128), 0)
    out = jnp.broadcast_to(rows[0], (8, 128))
    for k in range(1, 8):
        out = jnp.where(sublane == k, jnp.broadcast_to(rows[k], (8, 128)), out)
    return out


def tile_kernel(counts, tiles, idx_hbm, w0_ref, w1_ref, *refs):
    f32 = jnp.float32
    pieces, (out_ref, utab, stab, bufa, bufb, isem) = refs[: len(counts)], refs[len(counts) :]
    bufs = (bufa, bufb)
    steps = tiles // (2 * NT)

    def icopy(c, b):
        return pltpu.make_async_copy(idx_hbm.at[pl.ds(c * 2 * CH, 2 * CH)], bufs[b], isem.at[b])

    icopy(0, 0).start()
    icopy(1, 1).start()
    low = lax.broadcasted_iota(jnp.int32, (SHARD_S, 128), 1) < 64
    first_slot = 0
    for piece, count in zip(pieces, counts):

        def conv(i, carry, piece=piece, first_slot=first_slot):
            src = pl.multiple_of(i * SHARD, SHARD_S)
            slot = first_slot + i
            urow = pl.multiple_of(slot * SHARD_U, SHARD_U)
            srow = pl.multiple_of(slot * 2 * SHARD_S, 2 * SHARD_S)
            utab[pl.ds(urow, SHARD_U), :] = piece[pl.ds(src, SHARD_U), :].astype(f32)
            x = piece[pl.ds(src + SHARD_U, SHARD_S), :].astype(f32)
            r = pltpu.roll(x, 64, 1)
            stab[pl.ds(srow, SHARD_S), :] = jnp.where(low, x, r)
            stab[pl.ds(srow + SHARD_S, SHARD_S), :] = jnp.where(low, r, x)
            return carry

        lax.fori_loop(0, count, conv, 0)
        first_slot += count

    def tile(buf, j, t):
        w0 = w0_ref[pl.ds(t, 1), :]
        w1 = w1_ref[pl.ds(t, 1), :]
        w = jnp.concatenate([jnp.broadcast_to(w0, (64, 128)), jnp.broadcast_to(w1, (64, 128))], 0).T
        acc = jnp.zeros((8, 128), f32)
        for g in range(16):
            first = j * 128 + g * 8
            ur = merged([utab[pl.ds(buf[first + k], 1), :] for k in range(8)])
            sr = merged([stab[pl.ds(buf[CH + first + k], 1), :] for k in range(8)])
            acc = acc + ur * sr * w[g * 8 : (g + 1) * 8, :]
        out_ref[pl.ds(t, 1), :] = jnp.sum(acc, axis=0, keepdims=True)

    def body(i, carry):
        for b in range(2):
            c = i * 2 + b
            icopy(c, b).wait()
            for j in range(NT):
                tile(bufs[b], j, c * NT + j)

            @pl.when(i < steps - 1)
            def _():
                icopy(c + 2, b).start()

        return carry

    lax.fori_loop(0, steps, body, 0)


def slot_of(dev, color):
    me, grp = lax.axis_index("dev"), lax.axis_index("grp")
    dz = ((dev >> 3) - (me >> 3)) & 7
    dx = ((dev >> 1) - (me >> 1)) & 3
    ahead = (dz >= 1) & (dz <= 4)
    pair = jnp.where(ahead, dz - 1, (8 - dz) & 7)
    which = ahead.astype(jnp.int32)
    first = dx * 8 + ((pair - grp) & 3) * 2 + which
    second = ((3 - pair - grp) & 3) * 8 + dx * 2 + which
    far_side = (color ^ me) & 1
    return (far_side * 32 + jnp.where(color == 0, first, second)) * 2 + ((dev ^ color) & 1)


def tile_sums(pieces, nz_user, nz_sub, nz_value):
    tiles, width = nz_user.shape
    counts = tuple(p.shape[0] // SHARD for p in pieces)
    slots = sum(counts)
    user_row = slot_of(nz_user >> 10, (nz_user >> 8) & 1) * SHARD_U + (nz_user & 255)
    sub_row = (slot_of(nz_sub >> 8, (nz_sub >> 6) & 1) * 2 + ((nz_sub >> 7) & 1)) * SHARD_S + (nz_sub & 63)
    high = ((nz_user >> 9) & 1) == 1
    w1 = jnp.where(high, nz_value, 0.0)
    w0 = jnp.where(high, 0.0, nz_value)
    idx = jnp.concatenate([user_row.reshape(-1, 1, CH), sub_row.reshape(-1, 1, CH)], axis=1).reshape(-1)
    vmem = pl.BlockSpec(memory_space=pltpu.VMEM)
    out = pl.pallas_call(
        functools.partial(tile_kernel, counts, tiles),
        out_shape=jax.ShapeDtypeStruct((tiles, 128), jnp.float32),
        in_specs=[pl.BlockSpec(memory_space=pltpu.HBM), vmem, vmem] + [vmem] * len(pieces),
        out_specs=vmem,
        scratch_shapes=[
            pltpu.VMEM((slots * SHARD_U, 128), jnp.float32),
            pltpu.VMEM((slots * 2 * SHARD_S, 128), jnp.float32),
            pltpu.SMEM((2 * CH,), jnp.int32),
            pltpu.SMEM((2 * CH,), jnp.int32),
            pltpu.SemaphoreType.DMA((2,)),
        ],
        compiler_params=pltpu.CompilerParams(vmem_limit_bytes=32 * 2**20),
        name="tile_sums",
    )(idx, w0, w1, *pieces)
    return out[:, :64] + out[:, 64:]


def fetched(value, source):
    grps, devs = lax.axis_size("grp"), lax.axis_size("dev")
    pairs = []
    for g in range(grps):
        for d in range(devs):
            sg, sz, sx, sc = source(g, d // 8, d % 8 // 2, d % 2)
            pairs.append(((sg % 4) * devs + (sz % 8) * 8 + (sx % 4) * 2 + sc, g * devs + d))
    return lax.ppermute(value, ("grp", "dev"), pairs)


def swapped(value):
    return fetched(value, lambda g, z, x, c: (g, z, x, 1 - c))


def pair_of(g, c):
    return 3 - g if c else g


def near(step):
    return lambda g, z, x, c: (g, z, x + step, c) if c else (g + step, z, x, c)


def wide(step):
    return lambda g, z, x, c: (g + step, z, x, c) if c else (g, z, x + step, c)


def gathered(halves):
    core = lax.axis_index("dev") & 1
    keep = jnp.where(core == 0, halves[0], halves[1])
    give = jnp.where(core == 0, halves[1], halves[0])
    unit = jnp.concatenate([keep, swapped(give)], axis=0)
    back = fetched(unit, lambda g, z, x, c: (g, z - pair_of(g, c), x, c))
    ahead = fetched(unit, lambda g, z, x, c: (g, z + pair_of(g, c) + 1, x, c))
    pair = jnp.concatenate([back, ahead], axis=0)
    block = jnp.concatenate([pair] + [fetched(pair, near(k)) for k in (1, 2, 3)], axis=0)
    half = block.shape[0] // 2
    right, left = fetched(block, wide(1)), fetched(block, wide(-1))
    pieces = [block, right, fetched(right[:half], wide(1)), fetched(left[half:], wide(-1)), left]
    return pieces + [swapped(p) for p in pieces]


def packed(factor):
    rows = jnp.transpose(factor)
    half = rows.shape[0] // 2
    return jnp.concatenate([rows[:half], rows[half:]], axis=1)


def shards(nz_user, nz_sub, nz_value, tile_word, word_owner, user_factor, sub_factor):
    users, subs = packed(user_factor), packed(sub_factor)
    mine_a = jnp.concatenate([users[:SHARD_U], subs[:SHARD_S]], axis=0)
    mine_b = jnp.concatenate([users[SHARD_U:], subs[SHARD_S:]], axis=0)
    tile_rows = tile_sums(gathered((mine_a, mine_b)), nz_user, nz_sub, nz_value)
    tile_count, rank_width = tile_rows.shape
    grp_size = lax.axis_size("grp")
    dev_size = lax.axis_size("dev")
    devices_all = grp_size * dev_size
    words_total = word_owner.shape[0]
    words_local = words_total // devices_all
    out_rows = jnp.take(word_owner, tile_word)
    self_index = lax.axis_index("grp") * dev_size + lax.axis_index("dev")
    owner_dev = out_rows // words_local
    local_row = out_rows - owner_dev * words_local
    owned = owner_dev == self_index
    columns = jnp.arange(words_local, dtype=jnp.int32)
    own_table = (owned[:, None] & (local_row[:, None] == columns[None, :])).astype(jnp.float32)
    own_part = jnp.einsum("tr,tk->rk", tile_rows, own_table, precision=lax.Precision.HIGHEST)
    peer_ids = jnp.arange(devices_all, dtype=jnp.int32)
    outgoing = (jnp.logical_not(owned)[:, None] & (owner_dev[:, None] == peer_ids[None, :])).astype(
        jnp.float32
    )
    tile_ids = jnp.arange(tile_count, dtype=jnp.int32)
    earlier_table = (tile_ids[:, None] > tile_ids[None, :]).astype(jnp.float32)
    earlier = jnp.dot(
        earlier_table, outgoing, precision=lax.Precision.HIGHEST, preferred_element_type=jnp.float32
    )
    position = jnp.sum(earlier * outgoing, axis=1).astype(jnp.int32)
    send_slot = jnp.where(owned, devices_all * CAP, owner_dev * CAP + position)
    slot_ids = jnp.arange(devices_all * CAP, dtype=jnp.int32)
    slot_table = (send_slot[:, None] == slot_ids[None, :]).astype(jnp.float32)
    with_ids = jnp.concatenate(
        [tile_rows, (local_row + 1).astype(jnp.float32)[:, None], jnp.zeros((tile_count, 127 - rank_width), jnp.float32)],
        axis=1,
    )
    send = jnp.einsum("ts,tr->sr", slot_table, with_ids, precision=lax.Precision.HIGHEST)
    send = send.reshape(grp_size, dev_size, CAP * 128)
    got = exchange_both(send, ("dev", "grp"), ("dev", "grp"), (1, 0), (1, 0))
    got = got.reshape(devices_all * CAP, 128)
    got_rows = got[:, :rank_width]
    got_ids = got[:, rank_width].astype(jnp.int32) - 1
    got_table = (got_ids[:, None] == columns[None, :]).astype(jnp.float32)
    far_part = jnp.einsum("sr,sk->rk", got_rows, got_table, precision=lax.Precision.HIGHEST)
    return own_part + far_part


def solution(mesh):
    return jax.shard_map(
        shards,
        mesh=mesh,
        in_specs=(
            P(("grp", "dev"), None),
            P(("grp", "dev"), None),
            P(("grp", "dev"), None),
            P(("grp", "dev")),
            P(),
            P(None, "dev"),
            P(None, "dev"),
        ),
        out_specs=P(None, ("grp", "dev")),
        check_vma=False,
    )
```

```python
import functools

import jax
import jax.numpy as jnp
from jax import lax
from jax.experimental import pallas as pl
from jax.experimental.pallas import tpu as pltpu
from jax.sharding import PartitionSpec as P

CAP = 2


def cut_along(value, dim, peers):
    shape = value.shape
    pieces = value.reshape(*shape[:dim], peers, shape[dim] // peers, *shape[dim + 1 :])
    return jnp.moveaxis(pieces, dim, 0)


def joined_along(pieces, dim):
    pieces = jnp.moveaxis(pieces, 0, dim)
    shape = pieces.shape
    return pieces.reshape(*shape[:dim], shape[dim] * shape[dim + 1], *shape[dim + 2 :])


def exchange_both(value, axis, axes, splits, concats):
    sizes = [lax.axis_size(a) for a in axes]
    pieces = cut_along(value, splits[0], sizes[0])
    pieces = jnp.moveaxis(cut_along(pieces, splits[1] + 1, sizes[1]), 0, 1)
    inside = pieces.shape[2:]
    pieces = pieces.reshape(-1, *inside)
    pieces = lax.all_to_all(pieces, axis, split_axis=0, concat_axis=0, tiled=True)
    pieces = joined_along(pieces.reshape(*sizes, *inside), concats[0] + 1)
    return joined_along(pieces, concats[1])


NT = 8
CH = NT * 128
SHARD_U = 256
SHARD_S = 64
SHARD = SHARD_U + SHARD_S


def merged(rows):
    sublane = lax.broadcasted_iota(jnp.int32, (8, 128), 0)
    out = jnp.broadcast_to(rows[0], (8, 128))
    for k in range(1, 8):
        out = jnp.where(sublane == k, jnp.broadcast_to(rows[k], (8, 128)), out)
    return out


def tile_kernel(counts, tiles, idx_hbm, w0_ref, w1_ref, *refs):
    f32 = jnp.float32
    n = len(counts)
    pieces, (out_ref, utab, stab, stage, bufa, bufb, sem, isem) = refs[:n], refs[n:]
    bufs = (bufa, bufb)
    steps = tiles // (2 * NT)

    def icopy(c, b):
        return pltpu.make_async_copy(idx_hbm.at[pl.ds(c * 2 * CH, 2 * CH)], bufs[b], isem.at[b])

    icopy(0, 0).start()
    icopy(1, 1).start()
    starts = [sum(counts[:k]) for k in range(n)]

    def tcopy(k):
        rows = pl.ds(starts[k] * SHARD, counts[k] * SHARD)
        return pltpu.make_async_copy(pieces[k], stage.at[rows, :], sem.at[k])

    for k in range(n):
        tcopy(k).start()
    low = lax.broadcasted_iota(jnp.int32, (SHARD_S, 128), 1) < 64

    def conv(slot, carry):
        src = pl.multiple_of(slot * SHARD, SHARD_S)
        urow = pl.multiple_of(slot * SHARD_U, SHARD_U)
        srow = pl.multiple_of(slot * 2 * SHARD_S, 2 * SHARD_S)
        utab[pl.ds(urow, SHARD_U), :] = stage[pl.ds(src, SHARD_U), :].astype(f32)
        x = stage[pl.ds(src + SHARD_U, SHARD_S), :].astype(f32)
        r = pltpu.roll(x, 64, 1)
        stab[pl.ds(srow, SHARD_S), :] = jnp.where(low, x, r)
        stab[pl.ds(srow + SHARD_S, SHARD_S), :] = jnp.where(low, r, x)
        return carry

    for k in range(n):
        tcopy(k).wait()
        lax.fori_loop(starts[k], starts[k] + counts[k], conv, 0)

    def tile(buf, j, t):
        w0 = w0_ref[pl.ds(t, 1), :]
        w1 = w1_ref[pl.ds(t, 1), :]
        w = jnp.concatenate([jnp.broadcast_to(w0, (64, 128)), jnp.broadcast_to(w1, (64, 128))], 0).T
        acc = jnp.zeros((8, 128), f32)
        for g in range(16):
            first = j * 128 + g * 8
            ur = merged([utab[pl.ds(buf[first + k], 1), :] for k in range(8)])
            sr = merged([stab[pl.ds(buf[CH + first + k], 1), :] for k in range(8)])
            acc = acc + ur * sr * w[g * 8 : (g + 1) * 8, :]
        out_ref[pl.ds(t, 1), :] = jnp.sum(acc, axis=0, keepdims=True)

    def body(i, carry):
        for b in range(2):
            c = i * 2 + b
            icopy(c, b).wait()
            for j in range(NT):
                tile(bufs[b], j, c * NT + j)

            @pl.when(i < steps - 1)
            def _():
                icopy(c + 2, b).start()

        return carry

    lax.fori_loop(0, steps, body, 0)


def slot_of(dev, color):
    me, grp = lax.axis_index("dev"), lax.axis_index("grp")
    dz = ((dev >> 3) - (me >> 3)) & 7
    dx = ((dev >> 1) - (me >> 1)) & 3
    ahead = (dz >= 1) & (dz <= 4)
    pair = jnp.where(ahead, dz - 1, (8 - dz) & 7)
    which = ahead.astype(jnp.int32)
    first = which * 16 + dx * 4 + ((pair - grp) & 3)
    second = which * 16 + ((3 - pair - grp) & 3) * 4 + dx
    far_side = (color ^ me) & 1
    return (far_side * 32 + jnp.where(color == 0, first, second)) * 2 + ((dev ^ color) & 1)


def tile_sums(pieces, nz_user, nz_sub, nz_value):
    tiles, width = nz_user.shape
    counts = tuple(p.shape[0] // SHARD for p in pieces)
    slots = sum(counts)
    user_row = slot_of(nz_user >> 10, (nz_user >> 8) & 1) * SHARD_U + (nz_user & 255)
    sub_row = (slot_of(nz_sub >> 8, (nz_sub >> 6) & 1) * 2 + ((nz_sub >> 7) & 1)) * SHARD_S + (nz_sub & 63)
    high = ((nz_user >> 9) & 1) == 1
    w1 = jnp.where(high, nz_value, 0.0)
    w0 = jnp.where(high, 0.0, nz_value)
    idx = jnp.concatenate([user_row.reshape(-1, 1, CH), sub_row.reshape(-1, 1, CH)], axis=1).reshape(-1)
    vmem = pl.BlockSpec(memory_space=pltpu.VMEM)
    out = pl.pallas_call(
        functools.partial(tile_kernel, counts, tiles),
        out_shape=jax.ShapeDtypeStruct((tiles, 128), jnp.float32),
        in_specs=[pl.BlockSpec(memory_space=pltpu.HBM), vmem, vmem]
        + [pl.BlockSpec(memory_space=pltpu.HBM)] * len(pieces),
        out_specs=vmem,
        scratch_shapes=[
            pltpu.VMEM((slots * SHARD_U, 128), jnp.float32),
            pltpu.VMEM((slots * 2 * SHARD_S, 128), jnp.float32),
            pltpu.VMEM((slots * SHARD, 128), jnp.bfloat16),
            pltpu.SMEM((2 * CH,), jnp.int32),
            pltpu.SMEM((2 * CH,), jnp.int32),
            pltpu.SemaphoreType.DMA((len(pieces),)),
            pltpu.SemaphoreType.DMA((2,)),
        ],
        compiler_params=pltpu.CompilerParams(vmem_limit_bytes=44 * 2**20),
        name="tile_sums",
    )(idx, w0, w1, *pieces)
    return out[:, :64] + out[:, 64:]


def fetched(value, source):
    grps, devs = lax.axis_size("grp"), lax.axis_size("dev")
    pairs = []
    for g in range(grps):
        for d in range(devs):
            sg, sz, sx, sc = source(g, d // 8, d % 8 // 2, d % 2)
            pairs.append(((sg % 4) * devs + (sz % 8) * 8 + (sx % 4) * 2 + sc, g * devs + d))
    return lax.ppermute(value, ("grp", "dev"), pairs)


def swapped(value):
    return fetched(value, lambda g, z, x, c: (g, z, x, 1 - c))


def pair_of(g, c):
    return 3 - g if c else g


def near(step):
    return lambda g, z, x, c: (g, z, x + step, c) if c else (g + step, z, x, c)


def wide(step):
    return lambda g, z, x, c: (g + step, z, x, c) if c else (g, z, x + step, c)


def gathered(halves):
    core = lax.axis_index("dev") & 1
    keep = jnp.where(core == 0, halves[0], halves[1])
    give = jnp.where(core == 0, halves[1], halves[0])
    unit = jnp.concatenate([keep, swapped(give)], axis=0)
    back = fetched(unit, lambda g, z, x, c: (g, z - pair_of(g, c), x, c))
    ahead = fetched(unit, lambda g, z, x, c: (g, z + pair_of(g, c) + 1, x, c))
    a = jnp.concatenate([back] + [fetched(back, near(k)) for k in (1, 2, 3)], axis=0)
    right_a, left_a = fetched(a, wide(1)), fetched(a, wide(-1))
    b = jnp.concatenate([ahead] + [fetched(ahead, near(k)) for k in (1, 2, 3)], axis=0)
    left_b, right_b = fetched(b, wide(-1)), fetched(b, wide(1))
    pieces = [a, right_a, fetched(right_a, wide(1)), left_a, b, right_b, fetched(left_b, wide(-1)), left_b]
    return pieces + [swapped(p) for p in pieces]


def packed(factor):
    rows = jnp.transpose(factor)
    half = rows.shape[0] // 2
    return jnp.concatenate([rows[:half], rows[half:]], axis=1)


def shards(nz_user, nz_sub, nz_value, tile_word, word_owner, user_factor, sub_factor):
    users, subs = packed(user_factor), packed(sub_factor)
    mine_a = jnp.concatenate([users[:SHARD_U], subs[:SHARD_S]], axis=0)
    mine_b = jnp.concatenate([users[SHARD_U:], subs[SHARD_S:]], axis=0)
    tile_rows = tile_sums(gathered((mine_a, mine_b)), nz_user, nz_sub, nz_value)
    tile_count, rank_width = tile_rows.shape
    grp_size = lax.axis_size("grp")
    dev_size = lax.axis_size("dev")
    devices_all = grp_size * dev_size
    words_total = word_owner.shape[0]
    words_local = words_total // devices_all
    out_rows = jnp.take(word_owner, tile_word)
    self_index = lax.axis_index("grp") * dev_size + lax.axis_index("dev")
    owner_dev = out_rows // words_local
    local_row = out_rows - owner_dev * words_local
    owned = owner_dev == self_index
    columns = jnp.arange(words_local, dtype=jnp.int32)
    own_table = (owned[:, None] & (local_row[:, None] == columns[None, :])).astype(jnp.float32)
    own_part = jnp.einsum("tr,tk->rk", tile_rows, own_table, precision=lax.Precision.HIGHEST)
    peer_ids = jnp.arange(devices_all, dtype=jnp.int32)
    outgoing = (jnp.logical_not(owned)[:, None] & (owner_dev[:, None] == peer_ids[None, :])).astype(
        jnp.float32
    )
    tile_ids = jnp.arange(tile_count, dtype=jnp.int32)
    earlier_table = (tile_ids[:, None] > tile_ids[None, :]).astype(jnp.float32)
    earlier = jnp.dot(
        earlier_table, outgoing, precision=lax.Precision.HIGHEST, preferred_element_type=jnp.float32
    )
    position = jnp.sum(earlier * outgoing, axis=1).astype(jnp.int32)
    send_slot = jnp.where(owned, devices_all * CAP, owner_dev * CAP + position)
    slot_ids = jnp.arange(devices_all * CAP, dtype=jnp.int32)
    slot_table = (send_slot[:, None] == slot_ids[None, :]).astype(jnp.float32)
    with_ids = jnp.concatenate(
        [tile_rows, (local_row + 1).astype(jnp.float32)[:, None], jnp.zeros((tile_count, 127 - rank_width), jnp.float32)],
        axis=1,
    )
    send = jnp.einsum("ts,tr->sr", slot_table, with_ids, precision=lax.Precision.HIGHEST)
    send = send.reshape(grp_size, dev_size, CAP * 128)
    got = exchange_both(send, ("dev", "grp"), ("dev", "grp"), (1, 0), (1, 0))
    got = got.reshape(devices_all * CAP, 128)
    got_rows = got[:, :rank_width]
    got_ids = got[:, rank_width].astype(jnp.int32) - 1
    got_table = (got_ids[:, None] == columns[None, :]).astype(jnp.float32)
    far_part = jnp.einsum("sr,sk->rk", got_rows, got_table, precision=lax.Precision.HIGHEST)
    return own_part + far_part


def solution(mesh):
    return jax.shard_map(
        shards,
        mesh=mesh,
        in_specs=(
            P(("grp", "dev"), None),
            P(("grp", "dev"), None),
            P(("grp", "dev"), None),
            P(("grp", "dev")),
            P(),
            P(None, "dev"),
            P(None, "dev"),
        ),
        out_specs=P(None, ("grp", "dev")),
        check_vma=False,
    )
```

```python
import functools

import jax
import jax.numpy as jnp
from jax import lax
from jax.experimental import pallas as pl
from jax.experimental.pallas import tpu as pltpu
from jax.sharding import PartitionSpec as P

CAP = 2


def cut_along(value, dim, peers):
    shape = value.shape
    pieces = value.reshape(*shape[:dim], peers, shape[dim] // peers, *shape[dim + 1 :])
    return jnp.moveaxis(pieces, dim, 0)


def joined_along(pieces, dim):
    pieces = jnp.moveaxis(pieces, 0, dim)
    shape = pieces.shape
    return pieces.reshape(*shape[:dim], shape[dim] * shape[dim + 1], *shape[dim + 2 :])


def exchange_both(value, axis, axes, splits, concats):
    sizes = [lax.axis_size(a) for a in axes]
    pieces = cut_along(value, splits[0], sizes[0])
    pieces = jnp.moveaxis(cut_along(pieces, splits[1] + 1, sizes[1]), 0, 1)
    inside = pieces.shape[2:]
    pieces = pieces.reshape(-1, *inside)
    pieces = lax.all_to_all(pieces, axis, split_axis=0, concat_axis=0, tiled=True)
    pieces = joined_along(pieces.reshape(*sizes, *inside), concats[0] + 1)
    return joined_along(pieces, concats[1])


NT = 4
CH = NT * 128
SHARD_U = 256
SHARD_S = 64
SHARD = SHARD_U + SHARD_S


def merged(rows):
    sublane = lax.broadcasted_iota(jnp.int32, (8, 128), 0)
    out = jnp.broadcast_to(rows[0], (8, 128))
    for k in range(1, 8):
        out = jnp.where(sublane == k, jnp.broadcast_to(rows[k], (8, 128)), out)
    return out


def tile_kernel(counts, range_ref, idx_hbm, w0_ref, w1_ref, *refs):
    f32 = jnp.float32
    n = len(counts)
    pieces, (out_ref, utab, stab, stage, buf0, buf1, buf2, buf3, sem, isem) = refs[:n], refs[n:]
    bufs = (buf0, buf1, buf2, buf3)
    nb = len(bufs)
    c0, c1 = range_ref[0], range_ref[1]
    group0, group1 = c0 // nb, (c1 + nb - 1) // nb

    def icopy(c, b):
        rows = pl.ds(pl.multiple_of(c * 2 * CH, 2 * CH), 2 * CH)
        return pltpu.make_async_copy(idx_hbm.at[rows], bufs[b], isem.at[b])

    for b in range(nb):
        c = group0 * nb + b

        @pl.when((c >= c0) & (c < c1))
        def _():
            icopy(c, b).start()

    per = counts[0]

    def tcopy(source, k):
        rows = pl.ds(pl.multiple_of(k * per * SHARD, per * SHARD), per * SHARD)
        return pltpu.make_async_copy(source, stage.at[rows, :], sem.at[k])

    for k in range(n):
        tcopy(pieces[k], k).start()
    out_ref[...] = jnp.zeros_like(out_ref)
    low = lax.broadcasted_iota(jnp.int32, (SHARD_S, 128), 1) < 64

    def conv(k, carry):
        tcopy(pieces[0], k).wait()
        src = pl.multiple_of(k * per * SHARD, per * SHARD)
        urow = pl.multiple_of(k * per * SHARD_U, per * SHARD_U)
        srow = pl.multiple_of(k * per * 2 * SHARD_S, per * 2 * SHARD_S)
        for e in range(per):
            utab[pl.ds(urow + e * SHARD_U, SHARD_U), :] = stage[pl.ds(src + e * SHARD, SHARD_U), :].astype(f32)
            x = stage[pl.ds(src + e * SHARD + SHARD_U, SHARD_S), :].astype(f32)
            r = pltpu.roll(x, 64, 1)
            stab[pl.ds(srow + e * 2 * SHARD_S, SHARD_S), :] = jnp.where(low, x, r)
            stab[pl.ds(srow + (e * 2 + 1) * SHARD_S, SHARD_S), :] = jnp.where(low, r, x)
        return carry

    lax.fori_loop(0, n, conv, 0)

    def tile(buf, j, t):
        w0 = w0_ref[pl.ds(t, 1), :]
        w1 = w1_ref[pl.ds(t, 1), :]
        w = jnp.concatenate([jnp.broadcast_to(w0, (64, 128)), jnp.broadcast_to(w1, (64, 128))], 0).T
        acc = jnp.zeros((8, 128), f32)
        for g in range(16):
            first = j * 128 + g * 8
            ur = merged([utab[pl.ds(buf[first + k], 1), :] for k in range(8)])
            sr = merged([stab[pl.ds(buf[CH + first + k], 1), :] for k in range(8)])
            acc = acc + ur * sr * w[g * 8 : (g + 1) * 8, :]
        out_ref[pl.ds(t, 1), :] = jnp.sum(acc, axis=0, keepdims=True)

    def body(i, carry):
        for b in range(nb):
            c = i * nb + b

            @pl.when((c >= c0) & (c < c1))
            def _():
                icopy(c, b).wait()
                for j in range(NT):
                    tile(bufs[b], j, c * NT + j)

            @pl.when(c + nb < c1)
            def _():
                icopy(c + nb, b).start()

        return carry

    lax.fori_loop(group0, group1, body, 0)


def slot_of(dev, color):
    me, grp = lax.axis_index("dev"), lax.axis_index("grp")
    dz = ((dev >> 3) - (me >> 3)) & 7
    dx = ((dev >> 1) - (me >> 1)) & 3
    ahead = (dz >= 1) & (dz <= 4)
    pair = jnp.where(ahead, dz - 1, (8 - dz) & 7)
    which = ahead.astype(jnp.int32)
    first = which * 16 + dx * 4 + ((pair - grp) & 3)
    second = which * 16 + ((3 - pair - grp) & 3) * 4 + dx
    far_side = (color ^ me) & 1
    return (far_side * 32 + jnp.where(color == 0, first, second)) * 2 + ((dev ^ color) & 1)


def tile_inputs(nz_user, nz_sub, nz_value):
    user_row = slot_of(nz_user >> 10, (nz_user >> 8) & 1) * SHARD_U + (nz_user & 255)
    sub_row = (slot_of(nz_sub >> 8, (nz_sub >> 6) & 1) * 2 + ((nz_sub >> 7) & 1)) * SHARD_S + (nz_sub & 63)
    high = ((nz_user >> 9) & 1) == 1
    w1 = jnp.where(high, nz_value, 0.0)
    w0 = jnp.where(high, 0.0, nz_value)
    return jnp.concatenate([user_row.astype(jnp.float32), sub_row.astype(jnp.float32), w0, w1], axis=1)


def tile_sums(pieces, span, idx, w0, w1, name):
    tiles = w0.shape[0]
    counts = tuple(p.shape[0] // SHARD for p in pieces)
    slots = sum(counts)
    vmem = pl.BlockSpec(memory_space=pltpu.VMEM)
    hbm = pl.BlockSpec(memory_space=pltpu.HBM)
    out = pl.pallas_call(
        functools.partial(tile_kernel, counts),
        out_shape=jax.ShapeDtypeStruct((tiles, 128), jnp.float32),
        in_specs=[pl.BlockSpec(memory_space=pltpu.SMEM), hbm, vmem, vmem] + [hbm] * len(pieces),
        out_specs=vmem,
        scratch_shapes=[
            pltpu.VMEM((slots * SHARD_U, 128), jnp.float32),
            pltpu.VMEM((slots * 2 * SHARD_S, 128), jnp.float32),
            pltpu.VMEM((slots * SHARD, 128), jnp.bfloat16),
        ]
        + [pltpu.SMEM((2 * CH,), jnp.int32)] * 4
        + [pltpu.SemaphoreType.DMA((len(pieces),)), pltpu.SemaphoreType.DMA((4,))],
        compiler_params=pltpu.CompilerParams(vmem_limit_bytes=44 * 2**20),
        name=name,
    )(span, idx, w0, w1, *pieces)
    return out[:, :64] + out[:, 64:]


def fetched(value, source):
    grps, devs = lax.axis_size("grp"), lax.axis_size("dev")
    pairs = []
    for g in range(grps):
        for d in range(devs):
            sg, sz, sx, sc = source(g, d // 8, d % 8 // 2, d % 2)
            pairs.append(((sg % 4) * devs + (sz % 8) * 8 + (sx % 4) * 2 + sc, g * devs + d))
    return lax.ppermute(value, ("grp", "dev"), pairs)


def swapped(value):
    return fetched(value, lambda g, z, x, c: (g, z, x, 1 - c))


def pair_of(g, c):
    return 3 - g if c else g


def near(step):
    return lambda g, z, x, c: (g, z, x + step, c) if c else (g + step, z, x, c)


def wide(step):
    return lambda g, z, x, c: (g + step, z, x, c) if c else (g, z, x + step, c)


def gathered(halves):
    core = lax.axis_index("dev") & 1
    keep = jnp.where(core == 0, halves[0], halves[1])
    give = jnp.where(core == 0, halves[1], halves[0])
    unit = jnp.concatenate([keep, swapped(give)], axis=0)
    back = fetched(unit, lambda g, z, x, c: (g, z - pair_of(g, c), x, c))
    ahead = fetched(unit, lambda g, z, x, c: (g, z + pair_of(g, c) + 1, x, c))
    a = jnp.concatenate([back] + [fetched(back, near(k)) for k in (1, 2, 3)], axis=0)
    right_a, left_a = fetched(a, wide(1)), fetched(a, wide(-1))
    b = jnp.concatenate([ahead] + [fetched(ahead, near(k)) for k in (1, 2, 3)], axis=0)
    left_b, right_b = fetched(b, wide(-1)), fetched(b, wide(1))
    pieces = [a, right_a, fetched(right_a, wide(1)), left_a, b, right_b, fetched(left_b, wide(-1)), left_b]
    return pieces + [swapped(p) for p in pieces]


def packed(factor):
    rows = jnp.transpose(factor)
    half = rows.shape[0] // 2
    return jnp.concatenate([rows[:half], rows[half:]], axis=1)


def shards(nz_user, nz_sub, nz_value, tile_word, word_owner, user_factor, sub_factor):
    users, subs = packed(user_factor), packed(sub_factor)
    mine_a = jnp.concatenate([users[:SHARD_U], subs[:SHARD_S]], axis=0)
    mine_b = jnp.concatenate([users[SHARD_U:], subs[SHARD_S:]], axis=0)
    pieces = gathered((mine_a, mine_b))
    tile_count = nz_user.shape[0]
    rank_width = user_factor.shape[0]
    grp_size = lax.axis_size("grp")
    dev_size = lax.axis_size("dev")
    devices_all = grp_size * dev_size
    words_total = word_owner.shape[0]
    words_local = words_total // devices_all
    self_index = lax.axis_index("grp") * dev_size + lax.axis_index("dev")
    tile_ids = jnp.arange(tile_count, dtype=jnp.int32)
    rows_given = jnp.take(word_owner, tile_word)
    remote = (rows_given // words_local != self_index).astype(jnp.int32)
    remote_before = jnp.sum(jnp.where(tile_ids[:, None] < tile_ids[None, :], remote[:, None], 0), axis=0)
    remote_count = jnp.sum(remote)
    place = jnp.where(remote == 1, remote_before, remote_count + tile_ids - remote_before)
    order = (tile_ids[:, None] == place[None, :]).astype(jnp.float32)
    inputs = jnp.concatenate(
        [tile_inputs(nz_user, nz_sub, nz_value), rows_given.astype(jnp.float32)[:, None]], axis=1
    )
    inputs = jnp.dot(order, inputs, precision=lax.Precision.HIGHEST, preferred_element_type=jnp.float32)
    width = nz_user.shape[1]
    idx = inputs[:, : 2 * width].astype(jnp.int32).reshape(-1, NT, 2, width)
    idx = jnp.swapaxes(idx, 1, 2).reshape(-1)
    w0, w1 = inputs[:, 2 * width : 3 * width], inputs[:, 3 * width : 4 * width]
    out_rows = inputs[:, 4 * width].astype(jnp.int32)
    chunks = tile_count // NT
    first_span = jnp.stack([jnp.zeros_like(remote_count), (remote_count + NT - 1) // NT])
    second_span = jnp.stack([remote_count // NT, jnp.full_like(remote_count, chunks)])
    tile_rows = tile_sums(pieces, first_span, idx, w0, w1, "remote_tiles")
    own_rows = tile_sums(pieces, second_span, idx, w0, w1, "own_tiles")
    owner_dev = out_rows // words_local
    local_row = out_rows - owner_dev * words_local
    owned = owner_dev == self_index
    columns = jnp.arange(words_local, dtype=jnp.int32)
    own_table = (owned[:, None] & (local_row[:, None] == columns[None, :])).astype(jnp.float32)
    own_part = jnp.einsum("tr,tk->rk", own_rows, own_table, precision=lax.Precision.HIGHEST)
    peer_ids = jnp.arange(devices_all, dtype=jnp.int32)
    outgoing = (jnp.logical_not(owned)[:, None] & (owner_dev[:, None] == peer_ids[None, :])).astype(
        jnp.float32
    )
    earlier_table = (tile_ids[:, None] > tile_ids[None, :]).astype(jnp.float32)
    earlier = jnp.dot(
        earlier_table, outgoing, precision=lax.Precision.HIGHEST, preferred_element_type=jnp.float32
    )
    position = jnp.sum(earlier * outgoing, axis=1).astype(jnp.int32)
    send_slot = jnp.where(owned, devices_all * CAP, owner_dev * CAP + position)
    slot_ids = jnp.arange(devices_all * CAP, dtype=jnp.int32)
    slot_table = (send_slot[:, None] == slot_ids[None, :]).astype(jnp.float32)
    with_ids = jnp.concatenate(
        [tile_rows, (local_row + 1).astype(jnp.float32)[:, None], jnp.zeros((tile_count, 127 - rank_width), jnp.float32)],
        axis=1,
    )
    send = jnp.einsum("ts,tr->sr", slot_table, with_ids, precision=lax.Precision.HIGHEST)
    send = send.reshape(grp_size, dev_size, CAP * 128)
    got = exchange_both(send, ("dev", "grp"), ("dev", "grp"), (1, 0), (1, 0))
    got = got.reshape(devices_all * CAP, 128)
    got_rows = got[:, :rank_width]
    got_ids = got[:, rank_width].astype(jnp.int32) - 1
    got_table = (got_ids[:, None] == columns[None, :]).astype(jnp.float32)
    far_part = jnp.einsum("sr,sk->rk", got_rows, got_table, precision=lax.Precision.HIGHEST)
    return own_part + far_part


def solution(mesh):
    return jax.shard_map(
        shards,
        mesh=mesh,
        in_specs=(
            P(("grp", "dev"), None),
            P(("grp", "dev"), None),
            P(("grp", "dev"), None),
            P(("grp", "dev")),
            P(),
            P(None, "dev"),
            P(None, "dev"),
        ),
        out_specs=P(None, ("grp", "dev")),
        check_vma=False,
    )
```

```python
import functools

import jax
import jax.numpy as jnp
from jax import lax
from jax.experimental import pallas as pl
from jax.experimental.pallas import tpu as pltpu
from jax.sharding import PartitionSpec as P

CAP = 2


def cut_along(value, dim, peers):
    shape = value.shape
    pieces = value.reshape(*shape[:dim], peers, shape[dim] // peers, *shape[dim + 1 :])
    return jnp.moveaxis(pieces, dim, 0)


def joined_along(pieces, dim):
    pieces = jnp.moveaxis(pieces, 0, dim)
    shape = pieces.shape
    return pieces.reshape(*shape[:dim], shape[dim] * shape[dim + 1], *shape[dim + 2 :])


def exchange_both(value, axis, axes, splits, concats):
    sizes = [lax.axis_size(a) for a in axes]
    pieces = cut_along(value, splits[0], sizes[0])
    pieces = jnp.moveaxis(cut_along(pieces, splits[1] + 1, sizes[1]), 0, 1)
    inside = pieces.shape[2:]
    pieces = pieces.reshape(-1, *inside)
    pieces = lax.all_to_all(pieces, axis, split_axis=0, concat_axis=0, tiled=True)
    pieces = joined_along(pieces.reshape(*sizes, *inside), concats[0] + 1)
    return joined_along(pieces, concats[1])


NT = 8
CH = NT * 128
SHARD_U = 256
SHARD_S = 64
SHARD = SHARD_U + SHARD_S


def merged(rows):
    sublane = lax.broadcasted_iota(jnp.int32, (8, 128), 0)
    out = jnp.broadcast_to(rows[0], (8, 128))
    for k in range(1, 8):
        out = jnp.where(sublane == k, jnp.broadcast_to(rows[k], (8, 128)), out)
    return out


def tile_kernel(counts, tiles, idx_hbm, w0_ref, w1_ref, *refs):
    f32 = jnp.float32
    n = len(counts)
    pieces, (out_ref, utab, stab, stage, bufa, bufb, sem, isem) = refs[:n], refs[n:]
    bufs = (bufa, bufb)
    steps = tiles // (2 * NT)

    def icopy(c, b):
        return pltpu.make_async_copy(idx_hbm.at[pl.ds(c * 2 * CH, 2 * CH)], bufs[b], isem.at[b])

    icopy(0, 0).start()
    icopy(1, 1).start()
    per = counts[0]

    def tcopy(source, k):
        rows = pl.ds(pl.multiple_of(k * per * SHARD, per * SHARD), per * SHARD)
        return pltpu.make_async_copy(source, stage.at[rows, :], sem.at[k])

    for k in range(n):
        tcopy(pieces[k], k).start()
    low = lax.broadcasted_iota(jnp.int32, (SHARD_S, 128), 1) < 64

    def conv(k, carry):
        tcopy(pieces[0], k).wait()
        src = pl.multiple_of(k * per * SHARD, per * SHARD)
        urow = pl.multiple_of(k * per * SHARD_U, per * SHARD_U)
        srow = pl.multiple_of(k * per * 2 * SHARD_S, per * 2 * SHARD_S)
        for e in range(per):
            utab[pl.ds(urow + e * SHARD_U, SHARD_U), :] = stage[pl.ds(src + e * SHARD, SHARD_U), :].astype(f32)
            x = stage[pl.ds(src + e * SHARD + SHARD_U, SHARD_S), :].astype(f32)
            r = pltpu.roll(x, 64, 1)
            stab[pl.ds(srow + e * 2 * SHARD_S, SHARD_S), :] = jnp.where(low, x, r)
            stab[pl.ds(srow + (e * 2 + 1) * SHARD_S, SHARD_S), :] = jnp.where(low, r, x)
        return carry

    lax.fori_loop(0, n, conv, 0)

    def tile(buf, j, t):
        w0 = w0_ref[pl.ds(t, 1), :]
        w1 = w1_ref[pl.ds(t, 1), :]
        w = jnp.concatenate([jnp.broadcast_to(w0, (64, 128)), jnp.broadcast_to(w1, (64, 128))], 0).T
        acc = jnp.zeros((8, 128), f32)
        for g in range(16):
            first = j * 128 + g * 8
            ur = merged([utab[pl.ds(buf[first + k], 1), :] for k in range(8)])
            sr = merged([stab[pl.ds(buf[CH + first + k], 1), :] for k in range(8)])
            acc = acc + ur * sr * w[g * 8 : (g + 1) * 8, :]
        out_ref[pl.ds(t, 1), :] = jnp.sum(acc, axis=0, keepdims=True)

    def body(i, carry):
        for b in range(2):
            c = i * 2 + b
            icopy(c, b).wait()
            for j in range(NT):
                tile(bufs[b], j, c * NT + j)

            @pl.when(i < steps - 1)
            def _():
                icopy(c + 2, b).start()

        return carry

    lax.fori_loop(0, steps, body, 0)


def slot_of(dev, color):
    me, grp = lax.axis_index("dev"), lax.axis_index("grp")
    dz = ((dev >> 3) - (me >> 3)) & 7
    dx = ((dev >> 1) - (me >> 1)) & 3
    ahead = (dz >= 1) & (dz <= 4)
    pair = jnp.where(ahead, dz - 1, (8 - dz) & 7)
    which = ahead.astype(jnp.int32)
    first = which * 16 + dx * 4 + ((pair - grp) & 3)
    second = which * 16 + ((3 - pair - grp) & 3) * 4 + dx
    far_side = (color ^ me) & 1
    return (far_side * 32 + jnp.where(color == 0, first, second)) * 2 + ((dev ^ color) & 1)


def tile_sums(pieces, nz_user, nz_sub, nz_value):
    tiles, width = nz_user.shape
    counts = tuple(p.shape[0] // SHARD for p in pieces)
    slots = sum(counts)
    user_row = slot_of(nz_user >> 10, (nz_user >> 8) & 1) * SHARD_U + (nz_user & 255)
    sub_row = (slot_of(nz_sub >> 8, (nz_sub >> 6) & 1) * 2 + ((nz_sub >> 7) & 1)) * SHARD_S + (nz_sub & 63)
    high = ((nz_user >> 9) & 1) == 1
    w1 = jnp.where(high, nz_value, 0.0)
    w0 = jnp.where(high, 0.0, nz_value)
    idx = jnp.concatenate([user_row.reshape(-1, 1, CH), sub_row.reshape(-1, 1, CH)], axis=1).reshape(-1)
    vmem = pl.BlockSpec(memory_space=pltpu.VMEM)
    out = pl.pallas_call(
        functools.partial(tile_kernel, counts, tiles),
        out_shape=jax.ShapeDtypeStruct((tiles, 128), jnp.float32),
        in_specs=[pl.BlockSpec(memory_space=pltpu.HBM), vmem, vmem]
        + [pl.BlockSpec(memory_space=pltpu.HBM)] * len(pieces),
        out_specs=vmem,
        scratch_shapes=[
            pltpu.VMEM((slots * SHARD_U, 128), jnp.float32),
            pltpu.VMEM((slots * 2 * SHARD_S, 128), jnp.float32),
            pltpu.VMEM((slots * SHARD, 128), jnp.bfloat16),
            pltpu.SMEM((2 * CH,), jnp.int32),
            pltpu.SMEM((2 * CH,), jnp.int32),
            pltpu.SemaphoreType.DMA((len(pieces),)),
            pltpu.SemaphoreType.DMA((2,)),
        ],
        compiler_params=pltpu.CompilerParams(vmem_limit_bytes=44 * 2**20),
        name="tile_sums",
    )(idx, w0, w1, *pieces)
    return out[:, :64] + out[:, 64:]


def fetched(value, source):
    grps, devs = lax.axis_size("grp"), lax.axis_size("dev")
    pairs = []
    for g in range(grps):
        for d in range(devs):
            sg, sz, sx, sc = source(g, d // 8, d % 8 // 2, d % 2)
            pairs.append(((sg % 4) * devs + (sz % 8) * 8 + (sx % 4) * 2 + sc, g * devs + d))
    return lax.ppermute(value, ("grp", "dev"), pairs)


def swapped(value):
    return fetched(value, lambda g, z, x, c: (g, z, x, 1 - c))


def pair_of(g, c):
    return 3 - g if c else g


def near(step):
    return lambda g, z, x, c: (g, z, x + step, c) if c else (g + step, z, x, c)


def wide(step):
    return lambda g, z, x, c: (g + step, z, x, c) if c else (g, z, x + step, c)


def gathered(halves):
    core = lax.axis_index("dev") & 1
    keep = jnp.where(core == 0, halves[0], halves[1])
    give = jnp.where(core == 0, halves[1], halves[0])
    unit = jnp.concatenate([keep, swapped(give)], axis=0)
    back = fetched(unit, lambda g, z, x, c: (g, z - pair_of(g, c), x, c))
    ahead = fetched(unit, lambda g, z, x, c: (g, z + pair_of(g, c) + 1, x, c))
    a = jnp.concatenate([back] + [fetched(back, near(k)) for k in (1, 2, 3)], axis=0)
    right_a, left_a = fetched(a, wide(1)), fetched(a, wide(-1))
    b = jnp.concatenate([ahead] + [fetched(ahead, near(k)) for k in (1, 2, 3)], axis=0)
    left_b, right_b = fetched(b, wide(-1)), fetched(b, wide(1))
    pieces = [a, right_a, fetched(right_a, wide(1)), left_a, b, right_b, fetched(left_b, wide(-1)), left_b]
    return pieces + [swapped(p) for p in pieces]


def packed(factor):
    rows = jnp.transpose(factor)
    half = rows.shape[0] // 2
    return jnp.concatenate([rows[:half], rows[half:]], axis=1)


def shards(nz_user, nz_sub, nz_value, tile_word, word_owner, user_factor, sub_factor):
    users, subs = packed(user_factor), packed(sub_factor)
    mine_a = jnp.concatenate([users[:SHARD_U], subs[:SHARD_S]], axis=0)
    mine_b = jnp.concatenate([users[SHARD_U:], subs[SHARD_S:]], axis=0)
    tile_rows = tile_sums(gathered((mine_a, mine_b)), nz_user, nz_sub, nz_value)
    tile_count, rank_width = tile_rows.shape
    grp_size = lax.axis_size("grp")
    dev_size = lax.axis_size("dev")
    devices_all = grp_size * dev_size
    words_total = word_owner.shape[0]
    words_local = words_total // devices_all
    out_rows = jnp.take(word_owner, tile_word)
    self_index = lax.axis_index("grp") * dev_size + lax.axis_index("dev")
    owner_dev = out_rows // words_local
    local_row = out_rows - owner_dev * words_local
    owned = owner_dev == self_index
    columns = jnp.arange(words_local, dtype=jnp.int32)
    own_table = (owned[:, None] & (local_row[:, None] == columns[None, :])).astype(jnp.float32)
    own_part = jnp.einsum("tr,tk->rk", tile_rows, own_table, precision=lax.Precision.HIGHEST)
    peer_ids = jnp.arange(devices_all, dtype=jnp.int32)
    outgoing = (jnp.logical_not(owned)[:, None] & (owner_dev[:, None] == peer_ids[None, :])).astype(
        jnp.float32
    )
    tile_ids = jnp.arange(tile_count, dtype=jnp.int32)
    earlier_table = (tile_ids[:, None] > tile_ids[None, :]).astype(jnp.float32)
    earlier = jnp.dot(
        earlier_table, outgoing, precision=lax.Precision.HIGHEST, preferred_element_type=jnp.float32
    )
    position = jnp.sum(earlier * outgoing, axis=1).astype(jnp.int32)
    send_slot = jnp.where(owned, devices_all * CAP, owner_dev * CAP + position)
    slot_ids = jnp.arange(devices_all * CAP, dtype=jnp.int32)
    slot_table = (send_slot[:, None] == slot_ids[None, :]).astype(jnp.float32)
    with_ids = jnp.concatenate(
        [tile_rows, (local_row + 1).astype(jnp.float32)[:, None], jnp.zeros((tile_count, 127 - rank_width), jnp.float32)],
        axis=1,
    )
    send = jnp.einsum("ts,tr->sr", slot_table, with_ids, precision=lax.Precision.HIGHEST)
    send = send.reshape(grp_size, dev_size, CAP * 128)
    got = exchange_both(send, ("dev", "grp"), ("dev", "grp"), (1, 0), (1, 0))
    got = got.reshape(devices_all * CAP, 128)
    got_rows = got[:, :rank_width]
    got_ids = got[:, rank_width].astype(jnp.int32) - 1
    got_table = (got_ids[:, None] == columns[None, :]).astype(jnp.float32)
    far_part = jnp.einsum("sr,sk->rk", got_rows, got_table, precision=lax.Precision.HIGHEST)
    return own_part + far_part


def solution(mesh):
    return jax.shard_map(
        shards,
        mesh=mesh,
        in_specs=(
            P(("grp", "dev"), None),
            P(("grp", "dev"), None),
            P(("grp", "dev"), None),
            P(("grp", "dev")),
            P(),
            P(None, "dev"),
            P(None, "dev"),
        ),
        out_specs=P(None, ("grp", "dev")),
        check_vma=False,
    )
```

```python
import functools

import jax
import jax.numpy as jnp
from jax import lax
from jax.experimental import pallas as pl
from jax.experimental.pallas import tpu as pltpu
from jax.sharding import PartitionSpec as P

CAP = 2


NT = 8
CH = NT * 128
SHARD_U = 256
SHARD_S = 64
SHARD = SHARD_U + SHARD_S


def merged(rows):
    sublane = lax.broadcasted_iota(jnp.int32, (8, 128), 0)
    out = jnp.broadcast_to(rows[0], (8, 128))
    for k in range(1, 8):
        out = jnp.where(sublane == k, jnp.broadcast_to(rows[k], (8, 128)), out)
    return out


def tile_kernel(counts, tiles, dest_ref, ids_ref, idx_hbm, w0_ref, w1_ref, *refs):
    f32 = jnp.float32
    n = len(counts)
    pieces, (out_ref, utab, stab, stage, bufa, bufb, sem, isem) = refs[:n], refs[n:]
    bufs = (bufa, bufb)
    steps = tiles // (2 * NT)

    def icopy(c, b):
        return pltpu.make_async_copy(idx_hbm.at[pl.ds(c * 2 * CH, 2 * CH)], bufs[b], isem.at[b])

    icopy(0, 0).start()
    icopy(1, 1).start()
    per = counts[0]

    def tcopy(source, k):
        rows = pl.ds(pl.multiple_of(k * per * SHARD, per * SHARD), per * SHARD)
        return pltpu.make_async_copy(source, stage.at[rows, :], sem.at[k])

    for k in range(n):
        tcopy(pieces[k], k).start()
    out_ref[...] = jnp.zeros_like(out_ref)
    first_lanes = lax.broadcasted_iota(jnp.int32, (1, 128), 1) < 64
    low = lax.broadcasted_iota(jnp.int32, (SHARD_S, 128), 1) < 64

    def conv(k, carry):
        tcopy(pieces[0], k).wait()
        src = pl.multiple_of(k * per * SHARD, per * SHARD)
        urow = pl.multiple_of(k * per * SHARD_U, per * SHARD_U)
        srow = pl.multiple_of(k * per * 2 * SHARD_S, per * 2 * SHARD_S)
        for e in range(per):
            utab[pl.ds(urow + e * SHARD_U, SHARD_U), :] = stage[pl.ds(src + e * SHARD, SHARD_U), :].astype(f32)
            x = stage[pl.ds(src + e * SHARD + SHARD_U, SHARD_S), :].astype(f32)
            r = pltpu.roll(x, 64, 1)
            stab[pl.ds(srow + e * 2 * SHARD_S, SHARD_S), :] = jnp.where(low, x, r)
            stab[pl.ds(srow + (e * 2 + 1) * SHARD_S, SHARD_S), :] = jnp.where(low, r, x)
        return carry

    lax.fori_loop(0, n, conv, 0)

    def tile(buf, j, t):
        w0 = w0_ref[pl.ds(t, 1), :]
        w1 = w1_ref[pl.ds(t, 1), :]
        w = jnp.concatenate([jnp.broadcast_to(w0, (64, 128)), jnp.broadcast_to(w1, (64, 128))], 0).T
        acc = jnp.zeros((8, 128), f32)
        for g in range(16):
            first = j * 128 + g * 8
            ur = merged([utab[pl.ds(buf[first + k], 1), :] for k in range(8)])
            sr = merged([stab[pl.ds(buf[CH + first + k], 1), :] for k in range(8)])
            acc = acc + ur * sr * w[g * 8 : (g + 1) * 8, :]
        row = jnp.sum(acc, axis=0, keepdims=True)
        row = jnp.where(first_lanes, row + pltpu.roll(row, 64, 1), ids_ref[pl.ds(t, 1), :])
        to = pl.ds(dest_ref[t], 1)
        out_ref[to, :] = out_ref[to, :] + row

    def body(i, carry):
        for b in range(2):
            c = i * 2 + b
            icopy(c, b).wait()
            for j in range(NT):
                tile(bufs[b], j, c * NT + j)

            @pl.when(i < steps - 1)
            def _():
                icopy(c + 2, b).start()

        return carry

    lax.fori_loop(0, steps, body, 0)


NEAR_Z = (0, 1, -1, 2)
FAR_Z = (3, -2, 4, -3)
PAIR_CODE = sum(p << (2 * (z % 8)) for zs in (NEAR_Z, FAR_Z) for p, z in enumerate(zs))
WHICH_CODE = sum(1 << (z % 8) for z in FAR_Z)


def slot_of(dev, color):
    me, grp = lax.axis_index("dev"), lax.axis_index("grp")
    dz = ((dev >> 3) - (me >> 3)) & 7
    dx = ((dev >> 1) - (me >> 1)) & 3
    pair = (PAIR_CODE >> (2 * dz)) & 3
    which = (WHICH_CODE >> dz) & 1
    first = which * 16 + dx * 4 + ((pair - grp) & 3)
    second = which * 16 + ((3 - pair - grp) & 3) * 4 + dx
    far_side = (color ^ me) & 1
    return (far_side * 32 + jnp.where(color == 0, first, second)) * 2 + ((dev ^ color) & 1)


def tile_sums(pieces, dest, ids, out_rows, nz_user, nz_sub, nz_value):
    tiles, width = nz_user.shape
    counts = tuple(p.shape[0] // SHARD for p in pieces)
    slots = sum(counts)
    user_row = slot_of(nz_user >> 10, (nz_user >> 8) & 1) * SHARD_U + (nz_user & 255)
    sub_row = (slot_of(nz_sub >> 8, (nz_sub >> 6) & 1) * 2 + ((nz_sub >> 7) & 1)) * SHARD_S + (nz_sub & 63)
    high = ((nz_user >> 9) & 1) == 1
    w1 = jnp.where(high, nz_value, 0.0)
    w0 = jnp.where(high, 0.0, nz_value)
    idx = jnp.concatenate([user_row.reshape(-1, 1, CH), sub_row.reshape(-1, 1, CH)], axis=1).reshape(-1)
    vmem = pl.BlockSpec(memory_space=pltpu.VMEM)
    return pl.pallas_call(
        functools.partial(tile_kernel, counts, tiles),
        out_shape=jax.ShapeDtypeStruct((out_rows, 128), jnp.float32),
        in_specs=[pl.BlockSpec(memory_space=pltpu.SMEM), vmem, pl.BlockSpec(memory_space=pltpu.HBM), vmem, vmem]
        + [pl.BlockSpec(memory_space=pltpu.HBM)] * len(pieces),
        out_specs=vmem,
        scratch_shapes=[
            pltpu.VMEM((slots * SHARD_U, 128), jnp.float32),
            pltpu.VMEM((slots * 2 * SHARD_S, 128), jnp.float32),
            pltpu.VMEM((slots * SHARD, 128), jnp.bfloat16),
            pltpu.SMEM((2 * CH,), jnp.int32),
            pltpu.SMEM((2 * CH,), jnp.int32),
            pltpu.SemaphoreType.DMA((len(pieces),)),
            pltpu.SemaphoreType.DMA((2,)),
        ],
        compiler_params=pltpu.CompilerParams(vmem_limit_bytes=44 * 2**20),
        name="tile_sums",
    )(dest, ids, idx, w0, w1, *pieces)


def fetched(value, source):
    grps, devs = lax.axis_size("grp"), lax.axis_size("dev")
    pairs = []
    for g in range(grps):
        for d in range(devs):
            sg, sz, sx, sc = source(g, d // 8, d % 8 // 2, d % 2)
            pairs.append(((sg % 4) * devs + (sz % 8) * 8 + (sx % 4) * 2 + sc, g * devs + d))
    return lax.ppermute(value, ("grp", "dev"), pairs)


def swapped(value):
    return fetched(value, lambda g, z, x, c: (g, z, x, 1 - c))


def pair_of(g, c):
    return 3 - g if c else g


def near(step):
    return lambda g, z, x, c: (g, z, x + step, c) if c else (g + step, z, x, c)


def wide(step):
    return lambda g, z, x, c: (g + step, z, x, c) if c else (g, z, x + step, c)


def gathered(halves):
    core = lax.axis_index("dev") & 1
    keep = jnp.where(core == 0, halves[0], halves[1])
    give = jnp.where(core == 0, halves[1], halves[0])
    unit = jnp.concatenate([keep, swapped(give)], axis=0)
    back = fetched(unit, lambda g, z, x, c: (g, z + NEAR_Z[pair_of(g, c)], x, c))
    ahead = fetched(unit, lambda g, z, x, c: (g, z + FAR_Z[pair_of(g, c)], x, c))
    a = jnp.concatenate([back] + [fetched(back, near(k)) for k in (1, 2, 3)], axis=0)
    right_a, left_a = fetched(a, wide(1)), fetched(a, wide(-1))
    b = jnp.concatenate([ahead] + [fetched(ahead, near(k)) for k in (1, 2, 3)], axis=0)
    left_b, right_b = fetched(b, wide(-1)), fetched(b, wide(1))
    pieces = [a, right_a, fetched(right_a, wide(1)), left_a, b, right_b, fetched(left_b, wide(-1)), left_b]
    return pieces + [swapped(p) for p in pieces]


def packed(factor):
    rows = jnp.transpose(factor)
    half = rows.shape[0] // 2
    return jnp.concatenate([rows[:half], rows[half:]], axis=1)


def shards(nz_user, nz_sub, nz_value, tile_word, word_owner, user_factor, sub_factor):
    users, subs = packed(user_factor), packed(sub_factor)
    mine_a = jnp.concatenate([users[:SHARD_U], subs[:SHARD_S]], axis=0)
    mine_b = jnp.concatenate([users[SHARD_U:], subs[SHARD_S:]], axis=0)
    pieces = gathered((mine_a, mine_b))
    tile_count = nz_user.shape[0]
    rank_width = user_factor.shape[0]
    grp_size = lax.axis_size("grp")
    dev_size = lax.axis_size("dev")
    devices_all = grp_size * dev_size
    slots = devices_all * CAP
    words_local = word_owner.shape[0] // devices_all
    out_rows = jnp.take(word_owner, tile_word)
    self_index = lax.axis_index("grp") * dev_size + lax.axis_index("dev")
    owner_dev = out_rows // words_local
    local_row = out_rows - owner_dev * words_local
    owned = owner_dev == self_index
    tile_ids = jnp.arange(tile_count, dtype=jnp.int32)
    same = (owner_dev[:, None] == owner_dev[None, :]) & (tile_ids[:, None] < tile_ids[None, :])
    position = jnp.sum(same.astype(jnp.int32), axis=0)
    peer = (owner_dev % dev_size) * grp_size + owner_dev // dev_size
    dest = jnp.where(owned, slots + local_row, peer * CAP + position)
    lanes = jnp.arange(128, dtype=jnp.int32)
    ids = jnp.where(lanes[None, :] == rank_width, (local_row + 1)[:, None], 0).astype(jnp.float32)
    sums = tile_sums(pieces, dest, ids, slots + words_local, nz_user, nz_sub, nz_value)
    got = lax.all_to_all(
        sums[:slots].reshape(devices_all, 1, 1, CAP * 128), ("dev", "grp"), split_axis=0, concat_axis=0, tiled=True
    ).reshape(slots, 128)
    columns = jnp.arange(words_local, dtype=jnp.int32)
    got_ids = got[:, rank_width].astype(jnp.int32) - 1
    got_table = (got_ids[:, None] == columns[None, :]).astype(jnp.float32)
    far_part = jnp.einsum("sr,sk->rk", got[:, :rank_width], got_table, precision=lax.Precision.HIGHEST)
    return jnp.transpose(sums[slots:, :rank_width]) + far_part


def solution(mesh):
    return jax.shard_map(
        shards,
        mesh=mesh,
        in_specs=(
            P(("grp", "dev"), None),
            P(("grp", "dev"), None),
            P(("grp", "dev"), None),
            P(("grp", "dev")),
            P(),
            P(None, "dev"),
            P(None, "dev"),
        ),
        out_specs=P(None, ("grp", "dev")),
        check_vma=False,
    )
```

```python
import functools

import jax
import jax.numpy as jnp
from jax import lax
from jax.experimental import pallas as pl
from jax.experimental.pallas import tpu as pltpu
from jax.sharding import PartitionSpec as P

CAP = 2


NT = 8
CH = NT * 128
SHARD_U = 256
SHARD_S = 64
SHARD = SHARD_U + SHARD_S


def merged(rows):
    sublane = lax.broadcasted_iota(jnp.int32, (8, 128), 0)
    out = jnp.broadcast_to(rows[0], (8, 128))
    for k in range(1, 8):
        out = jnp.where(sublane == k, jnp.broadcast_to(rows[k], (8, 128)), out)
    return out


def tile_kernel(counts, tiles, dest_ref, ids_ref, idx_hbm, w0_ref, w1_ref, *refs):
    f32 = jnp.float32
    n = len(counts)
    pieces, (out_ref, rows_ref, send, utab, stab, stage, bufa, bufb, sem, isem) = refs[:n], refs[n:]
    bufs = (bufa, bufb)
    steps = tiles // (2 * NT)

    def icopy(c, b):
        return pltpu.make_async_copy(idx_hbm.at[pl.ds(c * 2 * CH, 2 * CH)], bufs[b], isem.at[b])

    icopy(0, 0).start()
    icopy(1, 1).start()
    per = counts[0]

    def tcopy(source, k):
        rows = pl.ds(pl.multiple_of(k * per * SHARD, per * SHARD), per * SHARD)
        return pltpu.make_async_copy(source, stage.at[rows, :], sem.at[k])

    for k in range(n):
        tcopy(pieces[k], k).start()
    send[...] = jnp.zeros_like(send)
    low = lax.broadcasted_iota(jnp.int32, (SHARD_S, 128), 1) < 64

    def conv(k, carry):
        tcopy(pieces[0], k).wait()
        src = pl.multiple_of(k * per * SHARD, per * SHARD)
        urow = pl.multiple_of(k * per * SHARD_U, per * SHARD_U)
        srow = pl.multiple_of(k * per * 2 * SHARD_S, per * 2 * SHARD_S)
        for e in range(per):
            utab[pl.ds(urow + e * SHARD_U, SHARD_U), :] = stage[pl.ds(src + e * SHARD, SHARD_U), :].astype(f32)
            x = stage[pl.ds(src + e * SHARD + SHARD_U, SHARD_S), :].astype(f32)
            r = pltpu.roll(x, 64, 1)
            stab[pl.ds(srow + e * 2 * SHARD_S, SHARD_S), :] = jnp.where(low, x, r)
            stab[pl.ds(srow + (e * 2 + 1) * SHARD_S, SHARD_S), :] = jnp.where(low, r, x)
        return carry

    lax.fori_loop(0, n, conv, 0)

    def tile(buf, j, t):
        w0 = w0_ref[pl.ds(t, 1), :]
        w1 = w1_ref[pl.ds(t, 1), :]
        w = jnp.concatenate([jnp.broadcast_to(w0, (64, 128)), jnp.broadcast_to(w1, (64, 128))], 0).T
        acc = jnp.zeros((8, 128), f32)
        for g in range(16):
            first = j * 128 + g * 8
            ur = merged([utab[pl.ds(buf[first + k], 1), :] for k in range(8)])
            sr = merged([stab[pl.ds(buf[CH + first + k], 1), :] for k in range(8)])
            acc = acc + ur * sr * w[g * 8 : (g + 1) * 8, :]
        rows_ref[pl.ds(t, 1), :] = jnp.sum(acc, axis=0, keepdims=True)

    def body(i, carry):
        for b in range(2):
            c = i * 2 + b
            icopy(c, b).wait()
            for j in range(NT):
                tile(bufs[b], j, c * NT + j)

            @pl.when(i < steps - 1)
            def _():
                icopy(c + 2, b).start()

        return carry

    lax.fori_loop(0, steps, body, 0)
    rows = rows_ref[...]
    first_lanes = lax.broadcasted_iota(jnp.int32, rows.shape, 1) < 64
    rows_ref[...] = jnp.where(first_lanes, rows + pltpu.roll(rows, 64, 1), ids_ref[...])

    def placed(i, carry):
        for j in range(16):
            send[pl.ds(dest_ref[i * 16 + j], 1), :] = rows_ref[pl.ds(i * 16 + j, 1), :]
        return carry

    lax.fori_loop(0, tiles // 16, placed, 0)
    out_ref[...] = send[: out_ref.shape[0], :]


NEAR_Z = (0, 1, -1, 2)
FAR_Z = (3, -2, 4, -3)
PAIR_CODE = sum(p << (2 * (z % 8)) for zs in (NEAR_Z, FAR_Z) for p, z in enumerate(zs))
WHICH_CODE = sum(1 << (z % 8) for z in FAR_Z)


def slot_of(dev, color):
    me, grp = lax.axis_index("dev"), lax.axis_index("grp")
    dz = ((dev >> 3) - (me >> 3)) & 7
    dx = ((dev >> 1) - (me >> 1)) & 3
    pair = (PAIR_CODE >> (2 * dz)) & 3
    which = (WHICH_CODE >> dz) & 1
    first = which * 16 + dx * 4 + ((pair - grp) & 3)
    second = which * 16 + ((3 - pair - grp) & 3) * 4 + dx
    far_side = (color ^ me) & 1
    return (far_side * 32 + jnp.where(color == 0, first, second)) * 2 + ((dev ^ color) & 1)


def tile_sums(pieces, dest, ids, send_rows, nz_user, nz_sub, nz_value):
    tiles, width = nz_user.shape
    counts = tuple(p.shape[0] // SHARD for p in pieces)
    slots = sum(counts)
    user_row = slot_of(nz_user >> 10, (nz_user >> 8) & 1) * SHARD_U + (nz_user & 255)
    sub_row = (slot_of(nz_sub >> 8, (nz_sub >> 6) & 1) * 2 + ((nz_sub >> 7) & 1)) * SHARD_S + (nz_sub & 63)
    high = ((nz_user >> 9) & 1) == 1
    w1 = jnp.where(high, nz_value, 0.0)
    w0 = jnp.where(high, 0.0, nz_value)
    idx = jnp.concatenate([user_row.reshape(-1, 1, CH), sub_row.reshape(-1, 1, CH)], axis=1).reshape(-1)
    vmem = pl.BlockSpec(memory_space=pltpu.VMEM)
    return pl.pallas_call(
        functools.partial(tile_kernel, counts, tiles),
        out_shape=[jax.ShapeDtypeStruct((rows, 128), jnp.float32) for rows in (send_rows, tiles)],
        in_specs=[pl.BlockSpec(memory_space=pltpu.SMEM), vmem, pl.BlockSpec(memory_space=pltpu.HBM), vmem, vmem]
        + [pl.BlockSpec(memory_space=pltpu.HBM)] * len(pieces),
        out_specs=[vmem, vmem],
        scratch_shapes=[
            pltpu.VMEM((send_rows + 8, 128), jnp.float32),
            pltpu.VMEM((slots * SHARD_U, 128), jnp.float32),
            pltpu.VMEM((slots * 2 * SHARD_S, 128), jnp.float32),
            pltpu.VMEM((slots * SHARD, 128), jnp.bfloat16),
            pltpu.SMEM((2 * CH,), jnp.int32),
            pltpu.SMEM((2 * CH,), jnp.int32),
            pltpu.SemaphoreType.DMA((len(pieces),)),
            pltpu.SemaphoreType.DMA((2,)),
        ],
        compiler_params=pltpu.CompilerParams(vmem_limit_bytes=44 * 2**20),
        name="tile_sums",
    )(dest, ids, idx, w0, w1, *pieces)


def fetched(value, source):
    grps, devs = lax.axis_size("grp"), lax.axis_size("dev")
    pairs = []
    for g in range(grps):
        for d in range(devs):
            sg, sz, sx, sc = source(g, d // 8, d % 8 // 2, d % 2)
            pairs.append(((sg % 4) * devs + (sz % 8) * 8 + (sx % 4) * 2 + sc, g * devs + d))
    return lax.ppermute(value, ("grp", "dev"), pairs)


def swapped(value):
    return fetched(value, lambda g, z, x, c: (g, z, x, 1 - c))


def pair_of(g, c):
    return 3 - g if c else g


def near(step):
    return lambda g, z, x, c: (g, z, x + step, c) if c else (g + step, z, x, c)


def wide(step):
    return lambda g, z, x, c: (g + step, z, x, c) if c else (g, z, x + step, c)


def gathered(halves):
    core = lax.axis_index("dev") & 1
    keep = jnp.where(core == 0, halves[0], halves[1])
    give = jnp.where(core == 0, halves[1], halves[0])
    unit = jnp.concatenate([keep, swapped(give)], axis=0)
    back = fetched(unit, lambda g, z, x, c: (g, z + NEAR_Z[pair_of(g, c)], x, c))
    ahead = fetched(unit, lambda g, z, x, c: (g, z + FAR_Z[pair_of(g, c)], x, c))
    a = jnp.concatenate([back] + [fetched(back, near(k)) for k in (1, 2, 3)], axis=0)
    right_a, left_a = fetched(a, wide(1)), fetched(a, wide(-1))
    b = jnp.concatenate([ahead] + [fetched(ahead, near(k)) for k in (1, 2, 3)], axis=0)
    left_b, right_b = fetched(b, wide(-1)), fetched(b, wide(1))
    pieces = [a, right_a, fetched(right_a, wide(1)), left_a, b, right_b, fetched(left_b, wide(-1)), left_b]
    return pieces + [swapped(p) for p in pieces]


def packed(factor):
    rows = jnp.transpose(factor)
    half = rows.shape[0] // 2
    return jnp.concatenate([rows[:half], rows[half:]], axis=1)


def shards(nz_user, nz_sub, nz_value, tile_word, word_owner, user_factor, sub_factor):
    users, subs = packed(user_factor), packed(sub_factor)
    mine_a = jnp.concatenate([users[:SHARD_U], subs[:SHARD_S]], axis=0)
    mine_b = jnp.concatenate([users[SHARD_U:], subs[SHARD_S:]], axis=0)
    pieces = gathered((mine_a, mine_b))
    tile_count = nz_user.shape[0]
    rank_width = user_factor.shape[0]
    grp_size = lax.axis_size("grp")
    dev_size = lax.axis_size("dev")
    devices_all = grp_size * dev_size
    slots = devices_all * CAP
    words_local = word_owner.shape[0] // devices_all
    out_rows = jnp.take(word_owner, tile_word)
    self_index = lax.axis_index("grp") * dev_size + lax.axis_index("dev")
    owner_dev = out_rows // words_local
    local_row = out_rows - owner_dev * words_local
    owned = owner_dev == self_index
    tile_ids = jnp.arange(tile_count, dtype=jnp.int32)
    same = (owner_dev[:, None] == owner_dev[None, :]) & (tile_ids[:, None] < tile_ids[None, :])
    position = jnp.sum(same.astype(jnp.int32), axis=0)
    peer = (owner_dev % dev_size) * grp_size + owner_dev // dev_size
    dest = jnp.where(owned, slots, peer * CAP + position)
    lanes = jnp.arange(128, dtype=jnp.int32)
    ids = jnp.where(lanes[None, :] == rank_width, (local_row + 1)[:, None], 0).astype(jnp.float32)
    send, sums = tile_sums(pieces, dest, ids, slots, nz_user, nz_sub, nz_value)
    got = lax.all_to_all(
        send.reshape(devices_all, 1, 1, CAP * 128), ("dev", "grp"), split_axis=0, concat_axis=0, tiled=True
    ).reshape(slots, 128)
    columns = jnp.arange(words_local, dtype=jnp.int32)
    own_table = (owned[:, None] & (local_row[:, None] == columns[None, :])).astype(jnp.float32)
    own_part = jnp.einsum("tr,tk->rk", sums[:, :rank_width], own_table, precision=lax.Precision.HIGHEST)
    got_ids = got[:, rank_width].astype(jnp.int32) - 1
    got_table = (got_ids[:, None] == columns[None, :]).astype(jnp.float32)
    far_part = jnp.einsum("sr,sk->rk", got[:, :rank_width], got_table, precision=lax.Precision.HIGHEST)
    return own_part + far_part


def solution(mesh):
    return jax.shard_map(
        shards,
        mesh=mesh,
        in_specs=(
            P(("grp", "dev"), None),
            P(("grp", "dev"), None),
            P(("grp", "dev"), None),
            P(("grp", "dev")),
            P(),
            P(None, "dev"),
            P(None, "dev"),
        ),
        out_specs=P(None, ("grp", "dev")),
        check_vma=False,
    )
```

```python
import functools

import jax
import jax.numpy as jnp
from jax import lax
from jax.experimental import pallas as pl
from jax.experimental.pallas import tpu as pltpu
from jax.sharding import PartitionSpec as P

CAP = 2


NT = 8
CH = NT * 128
SHARD_U = 256
SHARD_S = 64
SHARD = SHARD_U + SHARD_S


def merged(rows):
    sublane = lax.broadcasted_iota(jnp.int32, (8, 128), 0)
    out = jnp.broadcast_to(rows[0], (8, 128))
    for k in range(1, 8):
        out = jnp.where(sublane == k, jnp.broadcast_to(rows[k], (8, 128)), out)
    return out


def tile_kernel(counts, tiles, dest_ref, ids_ref, idx_hbm, w0_ref, w1_ref, *refs):
    f32 = jnp.float32
    n = len(counts)
    pieces, (out_ref, rows_ref, send, utab, stab, stage, bufa, bufb, sem, isem) = refs[:n], refs[n:]
    bufs = (bufa, bufb)
    steps = tiles // (2 * NT)

    def icopy(c, b):
        return pltpu.make_async_copy(idx_hbm.at[pl.ds(c * 2 * CH, 2 * CH)], bufs[b], isem.at[b])

    icopy(0, 0).start()
    icopy(1, 1).start()
    per = counts[0]

    def tcopy(source, k):
        rows = pl.ds(pl.multiple_of(k * per * SHARD, per * SHARD), per * SHARD)
        return pltpu.make_async_copy(source, stage.at[rows, :], sem.at[k])

    for k in range(n):
        tcopy(pieces[k], k).start()
    send[...] = jnp.zeros_like(send)
    low = lax.broadcasted_iota(jnp.int32, (SHARD_S, 128), 1) < 64

    def conv(k, carry):
        tcopy(pieces[0], k).wait()
        src = pl.multiple_of(k * per * SHARD, per * SHARD)
        urow = pl.multiple_of(k * per * SHARD_U, per * SHARD_U)
        srow = pl.multiple_of(k * per * 2 * SHARD_S, per * 2 * SHARD_S)
        for e in range(per):
            utab[pl.ds(urow + e * SHARD_U, SHARD_U), :] = stage[pl.ds(src + e * SHARD, SHARD_U), :].astype(f32)
            x = stage[pl.ds(src + e * SHARD + SHARD_U, SHARD_S), :].astype(f32)
            r = pltpu.roll(x, 64, 1)
            stab[pl.ds(srow + e * 2 * SHARD_S, SHARD_S), :] = jnp.where(low, x, r)
            stab[pl.ds(srow + (e * 2 + 1) * SHARD_S, SHARD_S), :] = jnp.where(low, r, x)
        return carry

    lax.fori_loop(0, n, conv, 0)

    def tile(buf, j, t):
        w0 = w0_ref[pl.ds(t, 1), :]
        w1 = w1_ref[pl.ds(t, 1), :]
        w = jnp.concatenate([jnp.broadcast_to(w0, (64, 128)), jnp.broadcast_to(w1, (64, 128))], 0).T
        acc = jnp.zeros((8, 128), f32)
        for g in range(16):
            first = j * 128 + g * 8
            ur = merged([utab[pl.ds(buf[first + k], 1), :] for k in range(8)])
            sr = merged([stab[pl.ds(buf[CH + first + k], 1), :] for k in range(8)])
            acc = acc + ur * sr * w[g * 8 : (g + 1) * 8, :]
        rows_ref[pl.ds(t, 1), :] = jnp.sum(acc, axis=0, keepdims=True)

    def body(i, carry):
        for b in range(2):
            c = i * 2 + b
            icopy(c, b).wait()
            for j in range(NT):
                tile(bufs[b], j, c * NT + j)

            @pl.when(i < steps - 1)
            def _():
                icopy(c + 2, b).start()

        return carry

    lax.fori_loop(0, steps, body, 0)
    rows = rows_ref[...]
    first_lanes = lax.broadcasted_iota(jnp.int32, rows.shape, 1) < 64
    rows_ref[...] = jnp.where(first_lanes, rows + pltpu.roll(rows, 64, 1), ids_ref[...])

    def placed(i, carry):
        for j in range(16):
            send[pl.ds(dest_ref[i * 16 + j], 1), :] = rows_ref[pl.ds(i * 16 + j, 1), :]
        return carry

    lax.fori_loop(0, tiles // 16, placed, 0)
    out_ref[...] = send[: out_ref.shape[0], :]


NEAR_Z = (0, 1, -1, 2)
FAR_Z = (3, -2, 4, -3)
PAIR_CODE = sum(p << (2 * (z % 8)) for zs in (NEAR_Z, FAR_Z) for p, z in enumerate(zs))
WHICH_CODE = sum(1 << (z % 8) for z in FAR_Z)


def slot_of(dev, color):
    me, grp = lax.axis_index("dev"), lax.axis_index("grp")
    dz = ((dev >> 3) - (me >> 3)) & 7
    dx = ((dev >> 1) - (me >> 1)) & 3
    pair = (PAIR_CODE >> (2 * dz)) & 3
    which = (WHICH_CODE >> dz) & 1
    first = which * 16 + dx * 4 + ((pair - grp) & 3)
    second = which * 16 + ((3 - pair - grp) & 3) * 4 + dx
    far_side = (color ^ me) & 1
    return (far_side * 32 + jnp.where(color == 0, first, second)) * 2 + ((dev ^ color) & 1)


def tile_inputs(nz_user, nz_sub, nz_value):
    user_row = slot_of(nz_user >> 10, (nz_user >> 8) & 1) * SHARD_U + (nz_user & 255)
    sub_row = (slot_of(nz_sub >> 8, (nz_sub >> 6) & 1) * 2 + ((nz_sub >> 7) & 1)) * SHARD_S + (nz_sub & 63)
    high = ((nz_user >> 9) & 1) == 1
    w1 = jnp.where(high, nz_value, 0.0)
    w0 = jnp.where(high, 0.0, nz_value)
    idx = jnp.concatenate([user_row.reshape(-1, 1, CH), sub_row.reshape(-1, 1, CH)], axis=1).reshape(-1)
    return idx, w0, w1


def tile_sums(pieces, dest, ids, idx, w0, w1, send_rows):
    tiles = w0.shape[0]
    counts = tuple(p.shape[0] // SHARD for p in pieces)
    slots = sum(counts)
    vmem = pl.BlockSpec(memory_space=pltpu.VMEM)
    return pl.pallas_call(
        functools.partial(tile_kernel, counts, tiles),
        out_shape=[jax.ShapeDtypeStruct((rows, 128), jnp.float32) for rows in (send_rows, tiles)],
        in_specs=[pl.BlockSpec(memory_space=pltpu.SMEM), vmem, pl.BlockSpec(memory_space=pltpu.HBM), vmem, vmem]
        + [pl.BlockSpec(memory_space=pltpu.HBM)] * len(pieces),
        out_specs=[vmem, vmem],
        scratch_shapes=[
            pltpu.VMEM((send_rows + 8, 128), jnp.float32),
            pltpu.VMEM((slots * SHARD_U, 128), jnp.float32),
            pltpu.VMEM((slots * 2 * SHARD_S, 128), jnp.float32),
            pltpu.VMEM((slots * SHARD, 128), jnp.bfloat16),
            pltpu.SMEM((2 * CH,), jnp.int32),
            pltpu.SMEM((2 * CH,), jnp.int32),
            pltpu.SemaphoreType.DMA((len(pieces),)),
            pltpu.SemaphoreType.DMA((2,)),
        ],
        compiler_params=pltpu.CompilerParams(vmem_limit_bytes=44 * 2**20),
        name="tile_sums",
    )(dest, ids, idx, w0, w1, *pieces)


def fetched(value, source):
    grps, devs = lax.axis_size("grp"), lax.axis_size("dev")
    pairs = []
    for g in range(grps):
        for d in range(devs):
            sg, sz, sx, sc = source(g, d // 8, d % 8 // 2, d % 2)
            pairs.append(((sg % 4) * devs + (sz % 8) * 8 + (sx % 4) * 2 + sc, g * devs + d))
    return lax.ppermute(value, ("grp", "dev"), pairs)


def swapped(value):
    return fetched(value, lambda g, z, x, c: (g, z, x, 1 - c))


def pair_of(g, c):
    return 3 - g if c else g


def near(step):
    return lambda g, z, x, c: (g, z, x + step, c) if c else (g + step, z, x, c)


def wide(step):
    return lambda g, z, x, c: (g + step, z, x, c) if c else (g, z, x + step, c)


def gathered(halves, given, prepare):
    core = lax.axis_index("dev") & 1
    keep = jnp.where(core == 0, halves[0], halves[1])
    give = jnp.where(core == 0, halves[1], halves[0])
    unit = jnp.concatenate([keep, swapped(give)], axis=0)
    unit, given = lax.optimization_barrier((unit, given))
    ready = prepare(*given)
    back = fetched(unit, lambda g, z, x, c: (g, z + NEAR_Z[pair_of(g, c)], x, c))
    ahead = fetched(unit, lambda g, z, x, c: (g, z + FAR_Z[pair_of(g, c)], x, c))
    back, ready = lax.optimization_barrier((back, ready))
    a = jnp.concatenate([back] + [fetched(back, near(k)) for k in (1, 2, 3)], axis=0)
    right_a, left_a = fetched(a, wide(1)), fetched(a, wide(-1))
    b = jnp.concatenate([ahead] + [fetched(ahead, near(k)) for k in (1, 2, 3)], axis=0)
    left_b, right_b = fetched(b, wide(-1)), fetched(b, wide(1))
    pieces = [a, right_a, fetched(right_a, wide(1)), left_a, b, right_b, fetched(left_b, wide(-1)), left_b]
    return pieces + [swapped(p) for p in pieces], ready


def packed(factor):
    rows = jnp.transpose(factor)
    half = rows.shape[0] // 2
    return jnp.concatenate([rows[:half], rows[half:]], axis=1)


def shards(nz_user, nz_sub, nz_value, tile_word, word_owner, user_factor, sub_factor):
    users, subs = packed(user_factor), packed(sub_factor)
    mine_a = jnp.concatenate([users[:SHARD_U], subs[:SHARD_S]], axis=0)
    mine_b = jnp.concatenate([users[SHARD_U:], subs[SHARD_S:]], axis=0)
    tile_count = nz_user.shape[0]
    rank_width = user_factor.shape[0]
    grp_size = lax.axis_size("grp")
    dev_size = lax.axis_size("dev")
    devices_all = grp_size * dev_size
    slots = devices_all * CAP
    words_local = word_owner.shape[0] // devices_all
    def prepare(nz_user, nz_sub, nz_value, tile_word):
        out_rows = jnp.take(word_owner, tile_word)
        self_index = lax.axis_index("grp") * dev_size + lax.axis_index("dev")
        owner_dev = out_rows // words_local
        local_row = out_rows - owner_dev * words_local
        owned = owner_dev == self_index
        tile_ids = jnp.arange(tile_count, dtype=jnp.int32)
        same = (owner_dev[:, None] == owner_dev[None, :]) & (tile_ids[:, None] < tile_ids[None, :])
        position = jnp.sum(same.astype(jnp.int32), axis=0)
        peer = (owner_dev % dev_size) * grp_size + owner_dev // dev_size
        dest = jnp.where(owned, slots, peer * CAP + position)
        lanes = jnp.arange(128, dtype=jnp.int32)
        ids = jnp.where(lanes[None, :] == rank_width, (local_row + 1)[:, None], 0).astype(jnp.float32)
        return dest, ids, owned, local_row, *tile_inputs(nz_user, nz_sub, nz_value)

    pieces, ready = gathered((mine_a, mine_b), (nz_user, nz_sub, nz_value, tile_word), prepare)
    dest, ids, owned, local_row, idx, w0, w1 = ready
    send, sums = tile_sums(pieces, dest, ids, idx, w0, w1, slots)
    got = lax.all_to_all(
        send.reshape(devices_all, 1, 1, CAP * 128), ("dev", "grp"), split_axis=0, concat_axis=0, tiled=True
    ).reshape(slots, 128)
    columns = jnp.arange(words_local, dtype=jnp.int32)
    own_table = (owned[:, None] & (local_row[:, None] == columns[None, :])).astype(jnp.float32)
    own_part = jnp.einsum("tr,tk->rk", sums[:, :rank_width], own_table, precision=lax.Precision.HIGHEST)
    got_ids = got[:, rank_width].astype(jnp.int32) - 1
    got_table = (got_ids[:, None] == columns[None, :]).astype(jnp.float32)
    far_part = jnp.einsum("sr,sk->rk", got[:, :rank_width], got_table, precision=lax.Precision.HIGHEST)
    return own_part + far_part


def solution(mesh):
    return jax.shard_map(
        shards,
        mesh=mesh,
        in_specs=(
            P(("grp", "dev"), None),
            P(("grp", "dev"), None),
            P(("grp", "dev"), None),
            P(("grp", "dev")),
            P(),
            P(None, "dev"),
            P(None, "dev"),
        ),
        out_specs=P(None, ("grp", "dev")),
        check_vma=False,
    )
```
